32 devices in a mesh: slab: 8 (over z, y), sub: 4 (over x, core).
Axes of the slice: x: 2, y: 2, z: 4, core: 2. Of those that a mesh axis runs over, the one named last changes fastest.
Arguments:
- coefficients: bfloat16 [7, 6, 6, 64, 12, 128], P(None, None, None, 'slab', 'sub'), may hold values from -1 to 1
- earlier: float32 [30, 6, 64, 12, 128], P(None, None, 'slab', 'sub'), may hold values from -6 to 6
- start: float32 [6, 64, 12, 128], P(None, 'slab', 'sub'), may hold values from -8 to 8
- shifts: float32 [5], replicated, may hold values from -0.3 to 0.3
Outputs:
- new_basis: float32 [6, 6, 64, 12, 128], P(None, None, 'slab', 'sub')
- projection: float32 [30, 6], replicated
- triangle: float32 [6, 6], replicated
The draws below stay inside these ranges and needn't reach their ends.
All inputs are finite; a program needn't handle non-finite values.
Results may differ from the reference program's by a relative error of at most 0.0015.
Values may be sent and summed in bfloat16 or wider, within the bound.
A program may use at most 64 MiB of HBM per device.

```python
import jax
import jax.numpy as jnp
from jax import lax

COMP = 6
STENCIL = 7
DEPTH = 5
BLOCK = 6
EARLIER = 30
NZ = 64
NX = 12
NY = 128


def earlier_basis(key):
    base_key = jax.random.fold_in(key, 7)
    dims = (EARLIER, COMP, NZ, NX, NY)
    values = jnp.clip(jax.random.normal(base_key, dims, jnp.float32), -6.0, 6.0)
    return values


def draw_earlier(key, part):
    return earlier_basis(key)


def draw_start(key, part):
    basis_values = earlier_basis(key)
    mixing = jnp.clip(jax.random.normal(jax.random.fold_in(key, 11), (EARLIER,), jnp.float32), -3.0, 3.0)
    jitter = jnp.clip(jax.random.normal(jax.random.fold_in(key, 13), (COMP, NZ, NX, NY), jnp.float32), -6.0, 6.0)
    combined = 0.3 * jnp.tensordot(mixing, basis_values, axes=1) + 0.5 * jitter
    return jnp.clip(combined, -8.0, 8.0)


def block_scale(stream_key, shape, pieces, least, largest):
    def one(axis_at, parts):
        draws = jax.random.uniform(jax.random.fold_in(jax.random.fold_in(stream_key, 6), axis_at), (parts,), jnp.float32, least / len(pieces), largest / len(pieces))
        return jnp.repeat(jnp.exp(draws), shape[axis_at] // parts).reshape((-1,) + (1,) * (len(shape) - axis_at - 1))

    loudness = one(*pieces[0])
    for cut in pieces[1:]:
        loudness = loudness * one(*cut)
    return loudness


def normal_values(stream_key, shape, scale, most, cuts=(), held_as=jnp.bfloat16):
    factor_of = block_scale(stream_key, shape, cuts, -0.22, 0.18) if cuts else 1.0
    values = jax.random.normal(stream_key, shape, jnp.float32) * scale * factor_of
    return jnp.minimum(jnp.maximum(values, -most), most).astype(held_as)


def setup_inputs(seed: int = 0) -> dict:
    key_of = jax.random.split(jax.random.key(seed), 5)
    return {
        "coefficients": normal_values(key_of[0], (STENCIL, COMP, COMP, NZ, NX, NY), (STENCIL * COMP) ** -0.5, 1.0, ((3, 8), (4, 4))),
        "earlier": draw_earlier(jax.random.fold_in(key_of[4], 71), 0),
        "start": draw_start(jax.random.fold_in(key_of[4], 71), 0),
        "shifts": jnp.clip(jax.random.uniform(key_of[3], (DEPTH,), jnp.float32, -0.3, 0.3), -0.3, 0.3),
    }


def nearby_fields(padded):
    center = padded[:, 1:-1, 1:-1]
    zeros_edge = jnp.zeros_like(center[..., :1])
    lower_y = jnp.concatenate([zeros_edge, center[..., :-1]], axis=3)
    upper_y = jnp.concatenate([center[..., 1:], zeros_edge], axis=3)
    return [center, padded[:, :-2, 1:-1], padded[:, 2:, 1:-1], padded[:, 1:-1, :-2], padded[:, 1:-1, 2:], lower_y, upper_y]

def apply_padded(coefficients, padded, theta):
    fields = nearby_fields(padded)
    result = (1.0 - theta) * fields[0]
    for coupling in range(len(fields)):
        result = result + jnp.sum(coefficients[coupling] * fields[coupling][None], axis=1)
    return result

def reference(coefficients, earlier, start, shifts):
    current = start
    vectors = [start]
    for step in range(DEPTH):
        padded = jnp.pad(current, ((0, 0), (1, 1), (1, 1), (0, 0)))
        current = apply_padded(coefficients, padded, shifts[step])
        vectors.append(current)
    basis = jnp.stack(vectors)
    flat = basis.reshape(BLOCK, -1)
    earlier_flat = earlier.reshape(EARLIER, -1)
    count = flat.shape[1]
    projection = jnp.dot(earlier_flat, flat.T, precision=lax.Precision.HIGHEST) / count
    rest = flat - jnp.dot(projection.T, earlier_flat, precision=lax.Precision.HIGHEST)
    gram = jnp.dot(rest, rest.T, precision=lax.Precision.HIGHEST) / count
    lower = jnp.linalg.cholesky(gram)
    new_flat = lax.linalg.triangular_solve(lower, rest, left_side=True, lower=True)
    return (new_flat.reshape(basis.shape), projection, lower.T)
```

```python
import functools

import jax
import jax.numpy as jnp
from jax import lax
from jax.experimental import pallas as pl
from jax.experimental.pallas import tpu as pltpu
from jax.sharding import PartitionSpec as P

MESH = pl.DeviceIdType.MESH
LANES = 128
ROWS = 8


def dot(a, b, nt=False):
    return lax.dot_general(
        a, b, (((1,), (1 if nt else 0,)), ((), ())),
        precision=lax.Precision.HIGHEST, preferred_element_type=jnp.float32,
    )


def iota(shape, dim):
    return lax.broadcasted_iota(jnp.int32, shape, dim)


def onehot(shape, test):
    return jnp.where(test(iota(shape, 0), iota(shape, 1)), 1.0, 0.0).astype(jnp.float32)


def diagonal(value):
    r, q = iota(value.shape, 0), iota(value.shape, 1)
    return jnp.where((r & 7) == (q & 7), value, 0.0)


def split(value):
    first = value.astype(jnp.bfloat16)
    left = value - first.astype(jnp.float32)
    second = left.astype(jnp.bfloat16)
    third = (left - second.astype(jnp.float32)).astype(jnp.bfloat16)
    return [first, second, third]


def dot_pieces(a, b, nt=False):
    found = None
    rows = a[0].shape[0]
    for at in (2, 1, 0):
        left = jnp.concatenate(a[: 3 - at], axis=0)
        part = lax.dot_general(
            left, b[at], (((1,), (1 if nt else 0,)), ((), ())),
            preferred_element_type=jnp.float32,
        )
        for i in reversed(range(3 - at)):
            piece = part[i * rows:(i + 1) * rows]
            found = piece if found is None else found + piece
    return found


def side_by_side(value):
    count, width = value.shape[0], value.shape[1]
    return jnp.concatenate(
        [value[:, x].reshape(count * ROWS, LANES) for x in range(width)], axis=1
    )


def factors(count):
    found = []
    while count > 1:
        fits = [f for f in range(2, min(count, 8) + 1) if count % f == 0]
        found.append(max(fits) if fits else count)
        count //= found[-1]
    return found


def stages_of(sizes):
    found = []
    for at, (_, count) in enumerate(sizes):
        stride = 1
        for size in factors(count):
            found.append(((stride, size), (1, 1)) if at == 0 else ((1, 1), (stride, size)))
            stride *= size
    return found


def joint_stages_of(sizes):
    slabs, subs = stages_of(sizes[:1]), [s[1] for s in stages_of((("", 1), sizes[1]))]
    first = slabs[0][0] if slabs else (1, 1)
    found = [(first, subs[0] if subs else (1, 1))]
    found += [(s[0], (1, 1)) for s in slabs[1:]] + [((1, 1), s) for s in subs[1:]]
    return found


def members(stage):
    return stage[0][1] * stage[1][1]


def offsets_of(stage):
    return [(a, b) for a in range(stage[0][1]) for b in range(stage[1][1]) if a or b]


def steps_of(depth):
    return ([1] if depth % 2 else []) + [2] * (depth // 2)


def lane_sums(value):
    return jnp.sum(value, axis=1, keepdims=True)


def sublane_sums(value):
    for shift in (4, 2, 1):
        value = value + pltpu.roll(value, shift, 0)
    return value


def inverse_root(value):
    scale = lax.rsqrt(value)
    return scale * (1.5 - 0.5 * value * scale * scale)


def kernel(
    sizes, coef_hbm, early_hbm, start_hbm, shifts_ref, new_ref, small_ref,
    coef_in, coef, edge_coef, gx_in, gz_send, gz_in, gz, allv, pieces, part, acc_ref,
    halo_x, halo_z, send_z, send_c, halo_c, pre_x, pre_z, ghost_x, ghost_z,
    ee, sums_ref, late_ref,
    mine_ee, gathered_ee, mine_b, gathered_b, mine_f, gathered_f,
    in_sem, face_send, face_recv, corner_send, corner_recv, g_send, g_recv,
    ee_send, ee_recv, b_send, b_recv, f_send, f_recv,
):
    depth = shifts_ref.shape[0]
    earlier, comp, width = early_hbm.shape[:3]
    block = depth + 1
    count = comp * width * ROWS * LANES * sizes[0][1] * sizes[1][1]
    half = LANES // 2
    rounds = steps_of(depth)
    single = stages_of(sizes)
    joint = joint_stages_of(sizes)
    place = [lax.axis_index(axis) for axis, _ in sizes]
    extent = [n for _, n in sizes]
    names = [axis for axis, _ in sizes]
    late = block - rounds[-1]
    lines = late // 2 + late % 2

    copy_start = pltpu.make_async_copy(start_hbm, allv.at[earlier], in_sem.at[0])
    copy_coef = pltpu.make_async_copy(coef_hbm, coef_in, in_sem.at[1])
    copy_early = pltpu.make_async_copy(early_hbm, allv.at[pl.ds(0, earlier)], in_sem.at[2])
    copy_start.start()
    copy_coef.start()
    copy_early.start()

    halo_x[...] = jnp.zeros_like(halo_x)
    halo_z[...] = jnp.zeros_like(halo_z)
    halo_c[...] = jnp.zeros_like(halo_c)
    gx_in[...] = jnp.zeros_like(gx_in)
    gz_in[...] = jnp.zeros_like(gz_in)

    def there(kind, side, sending):
        upward = (side == 0) == sending
        return place[kind] < extent[kind] - 1 if upward else place[kind] > 0

    def at_peer(dz, dx):
        return {names[0]: place[0] + dz, names[1]: place[1] + dx}

    def toward(side):
        return 1 if side == 0 else -1

    def peer(stage, offset):
        mine_at, peer_at, target = [], [], {}
        for axis in (0, 1):
            stride, size = stage[axis]
            digit = lax.rem(place[axis] // stride, size)
            other = lax.rem(digit + offset[axis], size)
            mine_at.append(digit)
            peer_at.append(other)
            target[names[axis]] = place[axis] + (other - digit) * stride
        flat = stage[1][1]
        return mine_at[0] * flat + mine_at[1], peer_at[0] * flat + peer_at[1], target

    barrier = pltpu.get_barrier_semaphore()
    expected = 0
    for stage in single + joint:
        for offset in offsets_of(stage):
            _, _, target = peer(stage, offset)
            pl.semaphore_signal(barrier, inc=1, device_id=target, device_id_type=MESH)
            expected += 1
    around = [(dz, dx) for dz in (-1, 0, 1) for dx in (-1, 0, 1) if dz or dx]
    beyond = around if len(joint) > 1 else []

    def exists(dz, dx):
        a = place[0] + dz
        b = place[1] + dx
        return (a >= 0) & (a < extent[0]) & (b >= 0) & (b < extent[1])

    for dz, dx in beyond:
        @pl.when(exists(dz, dx))
        def _():
            pl.semaphore_signal(barrier, inc=1, device_id=at_peer(dz, dx), device_id_type=MESH)

    send_z[...] = jnp.zeros_like(send_z)
    send_c[...] = jnp.zeros_like(send_c)
    edge_coef[...] = jnp.zeros_like(edge_coef)
    ee[...] = jnp.zeros_like(ee)
    sums_ref[...] = jnp.zeros_like(sums_ref)
    late_ref[...] = jnp.zeros_like(late_ref)

    def face_copy(r, step, what, kind, side):
        if kind == 0:
            src, dst = send_z.at[r, what, side], halo_z.at[r, what, side]
        else:
            x = width - 1 if side == 0 else 0
            src = allv.at[earlier + step, :, x] if what == 0 else part.at[r, :, x]
            dst = halo_x.at[r, what, side]
        dz, dx = (toward(side), 0) if kind == 0 else (0, toward(side))
        return pltpu.make_async_remote_copy(
            src_ref=src, dst_ref=dst,
            send_sem=face_send.at[r, what, kind, side],
            recv_sem=face_recv.at[r, what, kind, side],
            device_id=at_peer(dz, dx), device_id_type=MESH,
        )

    def corner_copy(r, sz, sx):
        return pltpu.make_async_remote_copy(
            src_ref=send_c.at[r, sz, sx], dst_ref=halo_c.at[r, sz, sx],
            send_sem=corner_send.at[r, sz, sx], recv_sem=corner_recv.at[r, sz, sx],
            device_id=at_peer(toward(sz), toward(sx)), device_id_type=MESH,
        )

    def g_copy(kind, side):
        if kind == 0:
            src, dst = gz_send.at[side], gz_in.at[side]
        else:
            src = coef_in.at[4, :, :, width - 1] if side == 0 else coef_in.at[3, :, :, 0]
            dst = gx_in.at[side]
        dz, dx = (toward(side), 0) if kind == 0 else (0, toward(side))
        return pltpu.make_async_remote_copy(
            src_ref=src, dst_ref=dst, send_sem=g_send.at[kind, side],
            recv_sem=g_recv.at[kind, side], device_id=at_peer(dz, dx), device_id_type=MESH,
        )

    def each_face(sending, kinds, act):
        for kind in kinds:
            for side in (0, 1):
                @pl.when(there(kind, side, sending))
                def _():
                    act(kind, side)

    def each_corner(sending, act):
        for sz in (0, 1):
            for sx in (0, 1):
                @pl.when(there(0, sz, sending) & there(1, sx, sending))
                def _():
                    act(sz, sx)

    def pack(r, what, source):
        for e in range(comp):
            for x in range(width):
                row = 4 * e + x
                tile = source(e, x)
                send_z[r, what, 0, row:row + 1, :] = tile[ROWS - 1:ROWS, :]
                send_z[r, what, 1, row:row + 1, :] = tile[0:1, :]

    def send_faces(r, step):
        pack(r, 0, lambda e, x: allv.at[earlier + step, e, x])
        each_face(True, (0, 1), lambda kind, side: face_copy(r, step, 0, kind, side).start())

    row2 = iota((ROWS, LANES), 0)
    row3 = iota((width, ROWS, LANES), 1)
    lane3 = iota((width, ROWS, LANES), 2)
    zero_tile = jnp.zeros((1, ROWS, LANES), jnp.float32)
    low_rows = row2 < 4

    def split_pair(below, above, odd):
        if odd:
            return jnp.where(low_rows, pltpu.roll(below, 4, 0), above)
        return jnp.where(low_rows, below, pltpu.roll(above, 4, 0))

    def pair_tile(ref, index, e):
        base = ROWS * (e // 2)
        return split_pair(
            ref[(*index, 0, slice(base, base + ROWS))],
            ref[(*index, 1, slice(base, base + ROWS))], e % 2,
        )

    def apply_local(step):
        acc = (1.0 - shifts_ref[step]) * allv[earlier + step]
        for e in range(comp):
            v = allv[earlier + step, e]
            near = [
                v,
                jnp.where(row3 > 0, pltpu.roll(v, 1, 1), 0.0),
                jnp.where(row3 < ROWS - 1, pltpu.roll(v, ROWS - 1, 1), 0.0),
                jnp.concatenate([zero_tile, v[:-1]], axis=0),
                jnp.concatenate([v[1:], zero_tile], axis=0),
                jnp.where(lane3 > 0, pltpu.roll(v, 1, 2), 0.0),
                jnp.where(lane3 < LANES - 1, pltpu.roll(v, LANES - 1, 2), 0.0),
            ]
            for d in range(len(near)):
                acc = acc + coef[d, :, e] * near[d][None]
        return acc

    def add_x(source, x_of):
        found = []
        for side, d, x in ((0, 3, 0), (1, 4, width - 1)):
            value = source(x)
            for e in range(comp):
                value = value + coef[d, :, e, x] * x_of(side, e)[None]
            found.append(value)
        return found

    def add_z(z_of):
        edge = jnp.zeros((comp, ROWS, LANES), jnp.float32)
        for e in range(comp):
            edge = edge + edge_coef[:, e] * z_of(e)[None]
        return edge

    def store_step(step, source, sides, edge):
        for c in range(comp):
            for x in range(width):
                value = sides[0][c] if x == 0 else sides[1][c] if x == width - 1 else source(x)[c]
                value = value + jnp.where(
                    row2 == 0, edge[c, x:x + 1, :],
                    jnp.where(row2 == ROWS - 1, edge[c, 4 + x:5 + x, :], 0.0),
                )
                allv[earlier + step, c, x] = value

    def take_faces(r, step, source):
        each_face(False, (1,), lambda kind, side: face_copy(r, step, 0, kind, side).wait_recv())
        sides = add_x(source, lambda side, e: halo_x[r, 0, side, e])
        each_face(False, (0,), lambda kind, side: face_copy(r, step, 0, kind, side).wait_recv())
        edge = add_z(lambda e: pair_tile(halo_z, (r, 0), e))
        store_step(step + 1, source, sides, edge)

    def cross_products(k, ref, base):
        total, group = earlier + k + 1, 6
        w = allv[earlier + k]
        for low in range(0, total, group):
            high = min(low + group, total)
            sums = jnp.sum(w[None] * allv[low:high], axis=(1, 2))
            ref[base + low:base + high, :] = jnp.sum(sums, axis=1)

    def as_line(value):
        return jnp.sum(value.T, axis=0, keepdims=True)

    def self_products(c):
        parts = split(side_by_side(allv[pl.ds(0, earlier), c]))
        for at, piece in enumerate(parts):
            pieces[at, c] = piece
        ee[...] += dot_pieces(parts, [parts[0], parts[1], parts[2]], nt=True)

    def self_finish():
        span = earlier * ROWS
        wide = dot(diagonal(ee[...]), onehot((span, LANES), lambda r, q: (r >> 3) == (q & 31)))
        wide = jnp.where((iota(wide.shape, 0) >> 6) == (iota(wide.shape, 1) >> 5), wide, 0.0)
        mine_ee[0] = dot(onehot((ROWS, span), lambda r, q: ((q >> 3) & 7) == r), wide)

    exchanges = {
        "ee": (single, mine_ee, gathered_ee, ee_send, ee_recv),
        "b": (joint, mine_b, gathered_b, b_send, b_recv),
        "f": (joint, mine_f, gathered_f, f_send, f_recv),
    }

    def begin(name, at):
        stages, own, slots, send_sem, recv_sem = exchanges[name]
        for offset in offsets_of(stages[at]):
            here, other, target = peer(stages[at], offset)
            pltpu.make_async_remote_copy(
                src_ref=own.at[at], dst_ref=slots.at[at, here],
                send_sem=send_sem.at[at, other], recv_sem=recv_sem.at[at, here],
                device_id=target, device_id_type=MESH,
            ).start()

    def finish(name, at):
        stages, own, slots, send_sem, recv_sem = exchanges[name]
        here, _, _ = peer(stages[at], (0, 0))
        slots[at, here] = own[at]
        for offset in offsets_of(stages[at]):
            _, other, target = peer(stages[at], offset)
            pltpu.make_async_remote_copy(
                src_ref=own.at[at], dst_ref=slots.at[at, other],
                send_sem=send_sem.at[at, other], recv_sem=recv_sem.at[at, other],
                device_id=target, device_id_type=MESH,
            ).wait_recv()
        whole = slots[at, 0]
        for other in range(1, members(stages[at])):
            whole = whole + slots[at, other]
        own[at + 1] = whole

    def drain(name):
        stages, own, slots, send_sem, recv_sem = exchanges[name]
        for at, stage in enumerate(stages):
            for offset in offsets_of(stage):
                here, other, target = peer(stage, offset)
                pltpu.make_async_remote_copy(
                    src_ref=own.at[at], dst_ref=slots.at[at, here],
                    send_sem=send_sem.at[at, other], recv_sem=recv_sem.at[at, here],
                    device_id=target, device_id_type=MESH,
                ).wait_send()

    def whole_exchange(name, first):
        stages = exchanges[name][0]
        for at in range(len(stages)):
            if at or not first:
                begin(name, at)
            finish(name, at)
        return exchanges[name][1][len(stages)] * (1.0 / count)

    def load_coefficients():
        @pl.loop(0, comp)
        def _(c):
            for d in range(coef.shape[0]):
                coef[d, c] = coef_in[d, c].astype(jnp.float32)
            for e in range(comp):
                for x in range(width):
                    edge_coef[c, e, x:x + 1, :] = coef[1, c, e, x, 0:1, :]
                    edge_coef[c, e, 4 + x:5 + x, :] = coef[2, c, e, x, ROWS - 1:ROWS, :]

        flat = comp * comp // 2
        for low in range(0, flat, 2):
            for side in (0, 1):
                both = []
                for at in (low, low + 1):
                    c, e = 2 * at // comp, 2 * at % comp
                    one, two = edge_coef[c, e], edge_coef[c, e + 1]
                    if side == 0:
                        both.append(jnp.where(low_rows, pltpu.roll(one, 4, 0), two))
                    else:
                        both.append(jnp.where(low_rows, one, pltpu.roll(two, 4, 0)))
                gz_send[side, ROWS * low:ROWS * (low + 2), :] = jnp.concatenate(
                    both, axis=0
                ).astype(jnp.bfloat16)

    def take_couplings():
        each_face(False, (0, 1), lambda kind, side: g_copy(kind, side).wait_recv())
        for low in range(0, comp * comp // 2, 2):
            below = gz_in[0, ROWS * low:ROWS * (low + 2), :].astype(jnp.float32)
            above = gz_in[1, ROWS * low:ROWS * (low + 2), :].astype(jnp.float32)
            for at in (0, 1):
                c, e = 2 * (low + at) // comp, 2 * (low + at) % comp
                b, a = below[ROWS * at:ROWS * (at + 1)], above[ROWS * at:ROWS * (at + 1)]
                gz[c, e] = split_pair(b, a, 0)
                gz[c, e + 1] = split_pair(b, a, 1)

    def complete_neighbours(r, step):
        for side, x in ((0, 0), (1, width - 1)):
            for c in range(comp):
                value = jnp.zeros((ROWS, LANES), jnp.float32)
                for e in range(comp):
                    value = value + gx_in[side, c, e].astype(jnp.float32) * allv[earlier + step, e, x]
                pre_x[side, c] = value
        total = jnp.zeros((comp, ROWS, LANES), jnp.float32)
        for e in range(comp):
            base = ROWS * (e // 2)
            own = split_pair(
                send_z[r, 0, 1, base:base + ROWS, :], send_z[r, 0, 0, base:base + ROWS, :], e % 2
            )
            total = total + gz[:, e] * own[None]
        pre_z[...] = total
        for sz in (0, 1):
            for sx in (0, 1):
                z = ROWS - 1 if sz == 0 else 0
                x = (4 if sz == 0 else 0) + (width - 1 if sx == 0 else 0)
                for c in range(comp):
                    send_c[r, sz, sx, c:c + 1, :] = pre_x[1 - sx, c, z:z + 1, :]
                    send_c[r, sz, sx, ROWS + c:ROWS + c + 1, :] = pre_z[c, x:x + 1, :]
        each_corner(True, lambda sz, sx: corner_copy(r, sz, sx).start())

    def take_ghosts(r, step):
        each_face(False, (1, 0), lambda kind, side: face_copy(r, step, 1, kind, side).wait_recv())
        each_corner(False, lambda sz, sx: corner_copy(r, sz, sx).wait_recv())
        for c in range(comp):
            value = pair_tile(halo_z, (r, 1), c) + pre_z[c]
            for sz in (0, 1):
                for sx in (0, 1):
                    row = (0 if sz == 0 else 4) + (0 if sx == 0 else width - 1)
                    value = value + jnp.where(row2 == row, halo_c[r, sz, sx, c:c + 1, :], 0.0)
            ghost_z[c] = value
            for side in (0, 1):
                value = halo_x[r, 1, side, c] + pre_x[side, c]
                for sz in (0, 1):
                    row = 0 if sz == 0 else ROWS - 1
                    value = value + jnp.where(
                        row2 == row, halo_c[r, sz, side, ROWS + c:ROWS + c + 1, :], 0.0
                    )
                ghost_x[side, c] = value

    copy_start.wait()
    for dz, dx in beyond:
        @pl.when(exists(dz, dx))
        def _():
            pl.semaphore_wait(barrier, 1)
    pl.semaphore_wait(barrier, expected)

    step = 0
    comps = list(range(comp))
    paired = [r for r, size in enumerate(rounds) if size == 2]
    per_round = -(-comp // max(1, len(rounds) - 1))
    done = 0
    ee_begun = False
    for r, size in enumerate(rounds):
        send_faces(r, step)
        if r == 0:
            copy_coef.wait()
            load_coefficients()
            each_face(True, (0, 1), lambda kind, side: g_copy(kind, side).start())
        if size == 2 and r == paired[0]:
            take_couplings()
        if size == 2:
            complete_neighbours(r, step)
        part[r] = apply_local(step)
        if size == 2:
            pack(r, 1, lambda e, x: part.at[r, e, x])
            each_face(True, (0, 1), lambda kind, side: face_copy(r, step, 1, kind, side).start())
        if r == 0:
            copy_early.wait()
        for k in range(done, min(step + 1, late)):
            cross_products(k, sums_ref.at[k // 2], (k % 2) * half)
            done = k + 1
        if done == late and r == len(rounds) - 1:
            for q in range(lines):
                mine_b[0, q] = as_line(sums_ref[q])
            begin("b", 0)
        todo, comps = comps[:per_round], comps[per_round:]
        if todo:
            @pl.loop(todo[0], todo[-1] + 1)
            def _(c):
                self_products(c)
        if ee_begun:
            finish("ee", 0)
            if len(single) > 1:
                begin("ee", 1)
            ee_begun = False
        if todo and not comps:
            self_finish()
            begin("ee", 0)
            ee_begun = len(rounds) - 1 > r
        take_faces(r, step, lambda x, r=r: part[r, :, x])
        if size == 2:
            if r == len(rounds) - 1:
                cross_products(step + 1, late_ref, 0)
            acc_ref[...] = apply_local(step + 1)
            take_ghosts(r, step)
            sides = add_x(lambda x: acc_ref[:, x], lambda side, e: ghost_x[side, e])
            edge = add_z(lambda e: ghost_z[e])
            store_step(step + 2, lambda x: acc_ref[:, x], sides, edge)
        step += size

    cross_products(depth, late_ref, half)
    mine_f[0] = as_line(late_ref[...])
    begin("f", 0)

    ee_from = 1 if len(single) > 1 else 0
    for at in range(ee_from, len(single)):
        if at > ee_from:
            begin("ee", at)
        finish("ee", at)
    packed = mine_ee[len(single)] * (1.0 / count)
    early = whole_exchange("b", True)

    row, lane = iota((ROWS, LANES), 0), iota((ROWS, LANES), 1)
    found = jnp.concatenate(
        [
            early[k // 2] if k % 2 == 0 else pltpu.roll(early[k // 2], half, 1)
            for k in range(late)
        ] + [jnp.zeros((ROWS - late, LANES), jnp.float32)], axis=0
    )
    proj_t = jnp.where(lane < earlier, found, 0.0)
    known = jnp.where(lane < earlier + row, found, 0.0)
    pick = onehot((ROWS, LANES), lambda r, q: q == r + earlier)
    gram = jnp.where(lane <= earlier + row, found, 0.0)
    gram = pltpu.roll(gram, LANES - earlier, 1)[:, :ROWS]
    square = jnp.concatenate(
        [packed] + [pltpu.roll(packed, LANES - 32 * g, 1) for g in range(1, 4)], axis=0
    )
    sr, sl = iota(square.shape, 0), iota(square.shape, 1)
    inside = (sl < earlier) & (sr < earlier)
    square = jnp.where(inside, square - jnp.where(sr == sl, 2.0, 0.0), 0.0)
    moved = dot(proj_t[:, :32], square) + pick
    gram = gram + dot(moved, known, nt=True)

    upper = gram
    inverse = onehot((ROWS, ROWS), lambda r, q: (r == q) & (r < late))
    r8 = iota((ROWS, ROWS), 0)
    q8 = iota((ROWS, ROWS), 1)
    for p in range(late):
        pivot = upper[p:p + 1, p:p + 1]
        scale = inverse_root(pivot)
        column = upper[:, p:p + 1] * scale
        row_u, row_i = upper[p:p + 1, :] * scale, inverse[p:p + 1, :] * scale
        upper = jnp.where(r8 == p, row_u, jnp.where(r8 > p, upper - column * row_u, upper))
        inverse = jnp.where(r8 == p, row_i, jnp.where(r8 > p, inverse - column * row_i, inverse))
    onto = dot(inverse, moved)

    mix = dot(inverse, pick - proj_t)
    tall = dot(onehot((late * ROWS, ROWS), lambda r, q: (r >> 3) == q), mix)
    span = earlier * ROWS
    mix = split(diagonal(dot(tall, onehot((LANES, span), lambda r, q: (q >> 3) == r))))
    weights = [
        [
            jnp.broadcast_to(
                tall[k * ROWS:(k + 1) * ROWS, earlier + i:earlier + i + 1], (ROWS, LANES)
            )
            for i in range(k + 1)
        ]
        for k in range(late)
    ]
    for c in range(comp):
        out = dot_pieces(mix, [pieces[at, c] for at in range(3)])
        for x in range(width):
            for k in range(late):
                value = out[k * ROWS:(k + 1) * ROWS, LANES * x:LANES * (x + 1)]
                for i in range(k + 1):
                    value = value + weights[k][i] * allv[earlier + i, c, x]
                new_ref[k, c, x] = value
    small_ref[0:ROWS, :] = proj_t
    small_ref[ROWS:2 * ROWS, :] = jnp.zeros((ROWS, LANES), jnp.float32)
    small_ref[ROWS:2 * ROWS, 0:ROWS] = jnp.where((q8 >= r8) & (r8 < late), upper, 0.0)

    final = whole_exchange("f", True)
    ys = [final, pltpu.roll(final, half, 1)][2 - (block - late):]
    spread = [jnp.broadcast_to(y, (ROWS, LANES)) for y in ys]
    tiles = -(-(earlier + block) // ROWS)
    columns = []
    for y in spread:
        col = [
            lane_sums(jnp.where(lane == row + ROWS * t, y, 0.0)) for t in range(tiles)
        ]
        img = [
            lane_sums(square[ROWS * t:ROWS * (t + 1)] * y) for t in range(square.shape[0] // ROWS)
        ]
        columns.append((col, img, lane_sums(onto * y)))
    wide = lambda value: jnp.broadcast_to(value, (ROWS, LANES))

    def inner(a, b):
        (col_a, _, r_a), (col_b, img_b, r_b) = columns[a], columns[b]
        total = -(r_a * r_b)
        for t in range(len(img_b)):
            total = total + jnp.where(row[:, :1] + ROWS * t < earlier, col_a[t] * img_b[t], 0.0)
        for t in range(tiles):
            total = total + jnp.where(row[:, :1] + ROWS * t == earlier + late + a, col_b[t], 0.0)
        return sublane_sums(wide(total))

    fresh = block - late
    scales, ratios, lines_out = [], {}, []
    for b in range(fresh):
        value = inner(b, b)
        for a in range(b):
            cross = inner(a, b)
            ratios[a, b] = cross * scales[a]
            value = value - ratios[a, b] * ratios[a, b]
        scales.append(inverse_root(value))
        ratios[b, b] = value * scales[b]
    triangle = small_ref[ROWS:2 * ROWS, :]
    proj_rows = small_ref[0:ROWS, :]
    for b in range(fresh):
        k = late + b
        triangle = triangle + jnp.where(lane == k, wide(columns[b][2]), 0.0)
        for a in range(b + 1):
            triangle = triangle + jnp.where((lane == k) & (row == late + a), ratios[a, b], 0.0)
        proj_rows = jnp.where((row == k) & (lane < earlier), spread[b], proj_rows)
    small_ref[ROWS:2 * ROWS, :] = triangle
    small_ref[0:ROWS, :] = proj_rows
    for b in range(fresh):
        for t in range(tiles):
            late_ref[b * half + ROWS * t:b * half + ROWS * (t + 1), :] = wide(columns[b][0][t])
        late_ref[b * half + ROWS * tiles:b * half + ROWS * (tiles + 1), :] = wide(columns[b][2])

    for c in range(comp):
        totals = [allv[earlier + late + b, c] for b in range(fresh)]
        for j in range(earlier):
            v = allv[j, c]
            for b in range(fresh):
                at = b * half + j
                totals[b] = totals[b] - late_ref[at:at + 1, :] * v
        for i in range(late):
            v = new_ref[i, c]
            for b in range(fresh):
                at = b * half + ROWS * tiles + i
                totals[b] = totals[b] - late_ref[at:at + 1, :] * v
        outs = []
        for b in range(fresh):
            value = totals[b]
            for a in range(b):
                value = value - ratios[a, b] * outs[a]
            outs.append(value * scales[b])
            new_ref[late + b, c] = outs[b]

    step = 0
    for r, size in enumerate(rounds):
        for what in range(size):
            each_face(
                True, (0, 1),
                lambda kind, side: face_copy(r, step, what, kind, side).wait_send(),
            )
        if size == 2:
            each_corner(True, lambda sz, sx: corner_copy(r, sz, sx).wait_send())
        step += size
    each_face(True, (0, 1), lambda kind, side: g_copy(kind, side).wait_send())
    for name in exchanges:
        drain(name)


def hand_over(rows, new_in, small, new_out, proj_out, tri_out, sem):
    copy = pltpu.make_async_copy(new_in, new_out, sem.at[0])
    copy.start()
    proj_out[...] = small[: proj_out.shape[0], : proj_out.shape[1]]
    tri_out[...] = small[rows:rows + tri_out.shape[0], : tri_out.shape[1]]
    copy.wait()


def body(sizes, coefficients, earlier, start, shifts):
    coefficients = jnp.transpose(coefficients, (0, 1, 2, 4, 3, 5))
    earlier = jnp.transpose(earlier, (0, 1, 3, 2, 4))
    start = jnp.transpose(start, (0, 2, 1, 3))
    depth, count = shifts.shape[0], earlier.shape[0]
    block = depth + 1
    kinds, comp, _, width, rows, lanes = coefficients.shape
    rounds = len(steps_of(depth))
    late = block - steps_of(depth)[-1]
    lines = late // 2 + late % 2
    single, joint = stages_of(sizes), joint_stages_of(sizes)
    most = max(members(stage) for stage in single)
    joined = max(members(stage) for stage in joint)
    f32, b16 = jnp.float32, jnp.bfloat16
    anywhere = pl.BlockSpec(memory_space=pl.ANY)
    vmem = pl.BlockSpec(memory_space=pltpu.VMEM)
    sems = pltpu.SemaphoreType.DMA
    new, small = pl.pallas_call(
        functools.partial(kernel, sizes),
        out_shape=(
            pltpu.VMEM((block, comp, width, rows, lanes), f32),
            pltpu.VMEM((2 * rows, lanes), f32),
        ),
        in_specs=[anywhere, anywhere, anywhere, pl.BlockSpec(memory_space=pltpu.SMEM)],
        out_specs=(vmem, vmem),
        scratch_shapes=[
            pltpu.VMEM(coefficients.shape, coefficients.dtype),
            pltpu.VMEM(coefficients.shape, f32),
            pltpu.VMEM((comp, comp, rows, lanes), f32),
            pltpu.VMEM((2, comp, comp, rows, lanes), b16),
            pltpu.VMEM((2, 4 * comp * comp, lanes), b16),
            pltpu.VMEM((2, 4 * comp * comp, lanes), b16),
            pltpu.VMEM((comp, comp, rows, lanes), f32),
            pltpu.VMEM((count + block, comp, width, rows, lanes), f32),
            pltpu.VMEM((3, comp, count * rows, width * lanes), b16),
            pltpu.VMEM((rounds, comp, width, rows, lanes), f32),
            pltpu.VMEM((comp, width, rows, lanes), f32),
            pltpu.VMEM((rounds, 2, 2, comp, rows, lanes), f32),
            pltpu.VMEM((rounds, 2, 2, 4 * comp, lanes), f32),
            pltpu.VMEM((rounds, 2, 2, 4 * comp, lanes), f32),
            pltpu.VMEM((rounds, 2, 2, 2 * rows, lanes), f32),
            pltpu.VMEM((rounds, 2, 2, 2 * rows, lanes), f32),
            pltpu.VMEM((2, comp, rows, lanes), f32),
            pltpu.VMEM((comp, rows, lanes), f32),
            pltpu.VMEM((2, comp, rows, lanes), f32),
            pltpu.VMEM((comp, rows, lanes), f32),
            pltpu.VMEM((count * rows, count * rows), f32),
            pltpu.VMEM((lines, lanes, lanes), f32),
            pltpu.VMEM((lanes, lanes), f32),
            pltpu.VMEM((len(single) + 1, rows, lanes), f32),
            pltpu.VMEM((len(single), most, rows, lanes), f32),
            pltpu.VMEM((len(joint) + 1, lines, 1, lanes), f32),
            pltpu.VMEM((len(joint), joined, lines, 1, lanes), f32),
            pltpu.VMEM((len(joint) + 1, 1, lanes), f32),
            pltpu.VMEM((len(joint), joined, 1, lanes), f32),
            sems((3,)),
            sems((rounds, 2, 2, 2)),
            sems((rounds, 2, 2, 2)),
            sems((rounds, 2, 2)),
            sems((rounds, 2, 2)),
            sems((2, 2)),
            sems((2, 2)),
            sems((len(single), most)),
            sems((len(single), most)),
            sems((len(joint), joined)),
            sems((len(joint), joined)),
            sems((len(joint), joined)),
            sems((len(joint), joined)),
        ],
        compiler_params=pltpu.CompilerParams(collective_id=0, has_side_effects=True),
        name="powers",
    )(coefficients, earlier, start, shifts)
    new = pltpu.with_memory_space_constraint(new, pltpu.VMEM)
    small = pltpu.with_memory_space_constraint(small, pltpu.VMEM)
    new, proj, tri = pl.pallas_call(
        functools.partial(hand_over, rows),
        out_shape=(
            jax.ShapeDtypeStruct(new.shape, f32),
            jax.ShapeDtypeStruct((block, count), f32),
            jax.ShapeDtypeStruct((block, block), f32),
        ),
        in_specs=[vmem, vmem],
        out_specs=(anywhere, vmem, vmem),
        scratch_shapes=[sems((1,))],
        name="hand_over",
    )(new, small)
    return jnp.transpose(new, (0, 1, 3, 2, 4)), proj.T, tri


def solution(mesh):
    sizes = (("slab", mesh.shape["slab"]), ("sub", mesh.shape["sub"]))
    placed = (
        P(None, None, None, "slab", "sub", None),
        P(None, None, "slab", "sub", None),
        P(None, "slab", "sub", None),
        P(),
    )
    return jax.shard_map(
        functools.partial(body, sizes),
        mesh=mesh,
        in_specs=placed,
        out_specs=(P(None, None, "slab", "sub", None), P(), P()),
        check_vma=False,
    )
```

```python
import functools

import jax
import jax.numpy as jnp
from jax import lax
from jax.experimental import pallas as pl
from jax.experimental.pallas import tpu as pltpu
from jax.sharding import PartitionSpec as P

MESH = pl.DeviceIdType.MESH
LANES = 128
ROWS = 8
REACH = (2, 1)


def dot(a, b, nt=False):
    return lax.dot_general(
        a, b, (((1,), (1 if nt else 0,)), ((), ())),
        precision=lax.Precision.HIGHEST, preferred_element_type=jnp.float32,
    )


def iota(shape, dim):
    return lax.broadcasted_iota(jnp.int32, shape, dim)


def onehot(shape, test):
    return jnp.where(test(iota(shape, 0), iota(shape, 1)), 1.0, 0.0).astype(jnp.float32)


def diagonal(value):
    r, q = iota(value.shape, 0), iota(value.shape, 1)
    return jnp.where((r & 7) == (q & 7), value, 0.0)


def split(value):
    first = value.astype(jnp.bfloat16)
    left = value - first.astype(jnp.float32)
    second = left.astype(jnp.bfloat16)
    third = (left - second.astype(jnp.float32)).astype(jnp.bfloat16)
    return [first, second, third]


def dot_pieces(a, b, nt=False):
    found = None
    rows = a[0].shape[0]
    for at in (2, 1, 0):
        left = jnp.concatenate(a[: 3 - at], axis=0)
        part = lax.dot_general(
            left, b[at], (((1,), (1 if nt else 0,)), ((), ())),
            preferred_element_type=jnp.float32,
        )
        for i in reversed(range(3 - at)):
            piece = part[i * rows:(i + 1) * rows]
            found = piece if found is None else found + piece
    return found


def side_by_side(value):
    count, width = value.shape[0], value.shape[1]
    return jnp.concatenate(
        [value[:, x].reshape(count * ROWS, LANES) for x in range(width)], axis=1
    )


def factors(count):
    found = []
    while count > 1:
        fits = [f for f in range(2, min(count, 8) + 1) if count % f == 0]
        found.append(max(fits) if fits else count)
        count //= found[-1]
    return found


def stages_of(sizes):
    found = []
    for at, (_, count) in enumerate(sizes):
        stride = 1
        for size in factors(count):
            found.append(((stride, size), (1, 1)) if at == 0 else ((1, 1), (stride, size)))
            stride *= size
    return found


def joint_stages_of(sizes):
    slabs, subs = stages_of(sizes[:1]), [s[1] for s in stages_of((("", 1), sizes[1]))]
    first = slabs[0][0] if slabs else (1, 1)
    found = [(first, subs[0] if subs else (1, 1))]
    found += [(s[0], (1, 1)) for s in slabs[1:]] + [((1, 1), s) for s in subs[1:]]
    return found


def levels_of(extent):
    levels = 0
    while any(reach << levels < n - 1 for reach, n in zip(REACH, extent)):
        levels += 1
    return levels


def members(stage):
    return stage[0][1] * stage[1][1]


def offsets_of(stage):
    return [(a, b) for a in range(stage[0][1]) for b in range(stage[1][1]) if a or b]


def steps_of(depth):
    return ([1] if depth % 2 else []) + [2] * (depth // 2)


def lane_sums(value):
    return jnp.sum(value, axis=1, keepdims=True)


def sublane_sums(value):
    for shift in (4, 2, 1):
        value = value + pltpu.roll(value, shift, 0)
    return value


def inverse_root(value):
    scale = lax.rsqrt(value)
    return scale * (1.5 - 0.5 * value * scale * scale)


def kernel(
    sizes, coef_hbm, early_hbm, start_hbm, shifts_hbm, new_ref, proj_ref, tri_ref,
    coef_in, coef, edge_coef, gx_in, gz_send, gz_in, gz, allv, pieces, part, acc_ref,
    halo_x, halo_z, send_z, send_c, halo_c, pre_x, pre_z, ghost_x, ghost_z,
    ee, ee_cross, sums_ref, late_ref, small_ref,
    mine_ee, gathered_ee, mine_b, gathered_b, mine_f, gathered_f,
    in_sem, face_send, face_recv, corner_send, corner_recv, g_send, g_recv,
    ee_send, ee_recv, b_send, b_recv, f_send, f_recv, ready, shifts_ref,
):
    depth = shifts_ref.shape[0]
    earlier, comp, width = early_hbm.shape[:3]
    block = depth + 1
    count = comp * width * ROWS * LANES * sizes[0][1] * sizes[1][1]
    half = LANES // 2
    rounds = steps_of(depth)
    single = stages_of(sizes)[::-1]
    joint = joint_stages_of(sizes)
    place = [lax.axis_index(axis) for axis, _ in sizes]
    extent = [n for _, n in sizes]
    names = [axis for axis, _ in sizes]
    late = block - rounds[-1]
    lines = late // 2 + late % 2

    copy_start = pltpu.make_async_copy(start_hbm, allv.at[earlier], in_sem.at[0])
    copy_coef = pltpu.make_async_copy(coef_hbm, coef_in, in_sem.at[1])
    copy_early = pltpu.make_async_copy(early_hbm, allv.at[pl.ds(0, earlier)], in_sem.at[2])
    copy_shifts = pltpu.make_async_copy(shifts_hbm, shifts_ref, in_sem.at[3])
    copy_start.start()
    copy_shifts.start()
    copy_coef.start()
    copy_early.start()

    def there(kind, side, sending):
        upward = (side == 0) == sending
        return place[kind] < extent[kind] - 1 if upward else place[kind] > 0

    def at_peer(dz, dx):
        return {names[0]: place[0] + dz, names[1]: place[1] + dx}

    def toward(side):
        return 1 if side == 0 else -1

    def peer(stage, offset):
        mine_at, peer_at, target = [], [], {}
        for axis in (0, 1):
            stride, size = stage[axis]
            digit = lax.rem(place[axis] // stride, size)
            other = lax.rem(digit + offset[axis], size)
            mine_at.append(digit)
            peer_at.append(other)
            target[names[axis]] = place[axis] + (other - digit) * stride
        flat = stage[1][1]
        return mine_at[0] * flat + mine_at[1], peer_at[0] * flat + peer_at[1], target

    levels = levels_of(extent)

    def around(reach, unit, act):
        for dz in range(-reach[0], reach[0] + 1):
            for dx in range(-reach[1], reach[1] + 1):
                far = (unit[0] * dz, unit[1] * dx)
                if far != (0, 0):
                    a, b = place[0] + far[0], place[1] + far[1]

                    @pl.when((a >= 0) & (a < extent[0]) & (b >= 0) & (b < extent[1]))
                    def _():
                        act(at_peer(*far))

    def signal(sem):
        return lambda where: pl.semaphore_signal(
            sem, inc=1, device_id=where, device_id_type=MESH
        )

    def wait_around(sem, reach, unit):
        total = 1
        for axis in (0, 1):
            seen = 1
            for d in range(1, reach[axis] + 1):
                far = d * unit[axis]
                seen = seen + jnp.where(place[axis] >= far, 1, 0)
                seen = seen + jnp.where(place[axis] + far < extent[axis], 1, 0)
            total = total * seen
        pl.semaphore_wait(sem, total - 1)

    def greet(level):
        if 0 < level <= levels:
            unit = tuple(x << (level - 1) for x in REACH)
            wait_around(ready.at[level - 1], (1, 1), unit)
        if level < levels:
            unit = tuple(x << level for x in REACH)
            around((1, 1), unit, signal(ready.at[level]))

    barrier = pltpu.get_barrier_semaphore()
    around(REACH, (1, 1), signal(barrier))

    for kind in (0, 1):
        for side in (0, 1):
            @pl.when(jnp.logical_not(there(kind, side, False)))
            def _():
                halo, coupling = (halo_z, gz_in) if kind == 0 else (halo_x, gx_in)
                for r in range(len(rounds)):
                    for what in (0, 1):
                        halo[r, what, side] = jnp.zeros_like(halo[r, what, side])
                coupling[side] = jnp.zeros_like(coupling[side])
    for sz in (0, 1):
        for sx in (0, 1):
            @pl.when(jnp.logical_not(there(0, sz, False) & there(1, sx, False)))
            def _():
                for r in range(len(rounds)):
                    halo_c[r, sz, sx] = jnp.zeros_like(halo_c[r, sz, sx])

    send_z[...] = jnp.zeros_like(send_z)
    send_c[...] = jnp.zeros_like(send_c)
    edge_coef[...] = jnp.zeros_like(edge_coef)
    ee[...] = jnp.zeros_like(ee)
    ee_cross[...] = jnp.zeros_like(ee_cross)
    sums_ref[...] = jnp.zeros_like(sums_ref)
    late_ref[...] = jnp.zeros_like(late_ref)

    def face_copy(r, step, what, kind, side):
        if kind == 0:
            src, dst = send_z.at[r, what, side], halo_z.at[r, what, side]
        else:
            x = width - 1 if side == 0 else 0
            src = allv.at[earlier + step, :, x] if what == 0 else part.at[r, :, x]
            dst = halo_x.at[r, what, side]
        dz, dx = (toward(side), 0) if kind == 0 else (0, toward(side))
        return pltpu.make_async_remote_copy(
            src_ref=src, dst_ref=dst,
            send_sem=face_send.at[what, kind, side],
            recv_sem=face_recv.at[r % 2, what, kind, side],
            device_id=at_peer(dz, dx), device_id_type=MESH,
        )

    def corner_copy(r, sz, sx):
        return pltpu.make_async_remote_copy(
            src_ref=send_c.at[r, sz, sx], dst_ref=halo_c.at[r, sz, sx],
            send_sem=corner_send.at[sz, sx], recv_sem=corner_recv.at[r % 2, sz, sx],
            device_id=at_peer(toward(sz), toward(sx)), device_id_type=MESH,
        )

    def g_copy(kind, side):
        if kind == 0:
            src, dst = gz_send.at[side], gz_in.at[side]
        else:
            src = coef_in.at[4, :, :, width - 1] if side == 0 else coef_in.at[3, :, :, 0]
            dst = gx_in.at[side]
        dz, dx = (toward(side), 0) if kind == 0 else (0, toward(side))
        return pltpu.make_async_remote_copy(
            src_ref=src, dst_ref=dst, send_sem=g_send.at[kind, side],
            recv_sem=g_recv.at[kind, side], device_id=at_peer(dz, dx), device_id_type=MESH,
        )

    def each_face(sending, kinds, act):
        for kind in kinds:
            for side in (0, 1):
                @pl.when(there(kind, side, sending))
                def _():
                    act(kind, side)

    def each_corner(sending, act):
        for sz in (0, 1):
            for sx in (0, 1):
                @pl.when(there(0, sz, sending) & there(1, sx, sending))
                def _():
                    act(sz, sx)

    def pack(r, what, source):
        for e in range(comp):
            for x in range(width):
                row = 4 * e + x
                tile = source(e, x)
                send_z[r, what, 0, row:row + 1, :] = tile[ROWS - 1:ROWS, :]
                send_z[r, what, 1, row:row + 1, :] = tile[0:1, :]

    def send_faces(r, step):
        pack(r, 0, lambda e, x: allv.at[earlier + step, e, x])
        each_face(True, (0, 1), lambda kind, side: face_copy(r, step, 0, kind, side).start())

    row2 = iota((ROWS, LANES), 0)
    row3 = iota((width, ROWS, LANES), 1)
    lane3 = iota((width, ROWS, LANES), 2)
    zero_tile = jnp.zeros((1, ROWS, LANES), jnp.float32)
    low_rows = row2 < 4

    def split_pair(below, above, odd):
        if odd:
            return jnp.where(low_rows, pltpu.roll(below, 4, 0), above)
        return jnp.where(low_rows, below, pltpu.roll(above, 4, 0))

    def pair_tile(ref, index, e):
        base = ROWS * (e // 2)
        return split_pair(
            ref[(*index, 0, slice(base, base + ROWS))],
            ref[(*index, 1, slice(base, base + ROWS))], e % 2,
        )

    def apply_local(step):
        acc = (1.0 - shifts_ref[step]) * allv[earlier + step]
        for e in range(comp):
            v = allv[earlier + step, e]
            near = [
                v,
                jnp.where(row3 > 0, pltpu.roll(v, 1, 1), 0.0),
                jnp.where(row3 < ROWS - 1, pltpu.roll(v, ROWS - 1, 1), 0.0),
                jnp.concatenate([zero_tile, v[:-1]], axis=0),
                jnp.concatenate([v[1:], zero_tile], axis=0),
                jnp.where(lane3 > 0, pltpu.roll(v, 1, 2), 0.0),
                jnp.where(lane3 < LANES - 1, pltpu.roll(v, LANES - 1, 2), 0.0),
            ]
            for d in range(len(near)):
                acc = acc + coef[d, :, e] * near[d][None]
        return acc

    def add_x(source, x_of):
        found = []
        for side, d, x in ((0, 3, 0), (1, 4, width - 1)):
            value = source(x)
            for e in range(comp):
                value = value + coef[d, :, e, x] * x_of(side, e)[None]
            found.append(value)
        return found

    def add_z(z_of):
        edge = jnp.zeros((comp, ROWS, LANES), jnp.float32)
        for e in range(comp):
            edge = edge + edge_coef[:, e] * z_of(e)[None]
        return edge

    def store_step(step, source, sides, edge):
        for c in range(comp):
            for x in range(width):
                value = sides[0][c] if x == 0 else sides[1][c] if x == width - 1 else source(x)[c]
                value = value + jnp.where(
                    row2 == 0, edge[c, x:x + 1, :],
                    jnp.where(row2 == ROWS - 1, edge[c, 4 + x:5 + x, :], 0.0),
                )
                allv[earlier + step, c, x] = value

    def take_faces(r, step, source):
        each_face(False, (1,), lambda kind, side: face_copy(r, step, 0, kind, side).wait_recv())
        sides = add_x(source, lambda side, e: halo_x[r, 0, side, e])
        each_face(False, (0,), lambda kind, side: face_copy(r, step, 0, kind, side).wait_recv())
        edge = add_z(lambda e: pair_tile(halo_z, (r, 0), e))
        store_step(step + 1, source, sides, edge)

    def cross_products(k, ref, base):
        total, group = earlier + k + 1, 6
        w = allv[earlier + k]
        for low in range(0, total, group):
            high = min(low + group, total)
            sums = jnp.sum(w[None] * allv[low:high], axis=(1, 2))
            ref[base + low:base + high, :] = jnp.sum(sums, axis=1)

    def as_line(value):
        return jnp.sum(value.T, axis=0, keepdims=True)

    def times(a, b):
        return lax.dot_general(
            a, b, (((1,), (1,)), ((), ())), preferred_element_type=jnp.float32
        )

    def self_products(c):
        parts = split(side_by_side(allv[pl.ds(0, earlier), c]))
        for at, piece in enumerate(parts):
            pieces[at, c] = piece
        one = times(parts[0], parts[0])
        two = times(jnp.concatenate(parts[:2], axis=0), parts[1])
        three = times(parts[0], parts[2])
        span = earlier * ROWS
        ee[...] += one + two[span:]
        ee_cross[...] += two[:span] + three

    def gather_self(value):
        span = earlier * ROWS
        rows = jnp.sum(diagonal(value).reshape(earlier, ROWS, span), axis=1)
        own = onehot((span, LANES), lambda r, q: (r >> 3) == q).astype(jnp.bfloat16)
        found = None
        for piece in split(rows)[::-1]:
            some = lax.dot_general(
                piece, own, (((1,), (0,)), ((), ())), preferred_element_type=jnp.float32
            )
            found = some if found is None else found + some
        return jnp.concatenate(
            [found, jnp.zeros((LANES - earlier, LANES), jnp.float32)], axis=0
        )

    def self_finish():
        cross = gather_self(ee_cross[...])
        whole = gather_self(ee[...])[:32] + (cross + cross.T)[:32]
        packed = whole[:ROWS]
        for g in range(1, 4):
            packed = packed + pltpu.roll(whole[ROWS * g:ROWS * (g + 1)], 32 * g, 1)
        mine_ee[0] = packed

    exchanges = {
        "ee": (single, mine_ee, gathered_ee, ee_send, ee_recv),
        "b": (joint, mine_b, gathered_b, b_send, b_recv),
        "f": (joint, mine_f, gathered_f, f_send, f_recv),
    }

    def begin(name, at):
        stages, own, slots, send_sem, recv_sem = exchanges[name]
        for offset in offsets_of(stages[at]):
            here, _, target = peer(stages[at], offset)
            pltpu.make_async_remote_copy(
                src_ref=own.at[at], dst_ref=slots.at[at, here],
                send_sem=send_sem.at[at], recv_sem=recv_sem.at[at],
                device_id=target, device_id_type=MESH,
            ).start()

    def all_of(name, at):
        stages, own, slots, send_sem, recv_sem = exchanges[name]
        others = slots.at[at, pl.ds(0, members(stages[at]) - 1)]
        _, _, target = peer(stages[at], offsets_of(stages[at])[0])
        return pltpu.make_async_remote_copy(
            src_ref=others, dst_ref=others, send_sem=send_sem.at[at], recv_sem=recv_sem.at[at],
            device_id=target, device_id_type=MESH,
        )

    def finish(name, at):
        stages, own, slots, _, _ = exchanges[name]
        here, _, _ = peer(stages[at], (0, 0))
        slots[at, here] = own[at]
        all_of(name, at).wait_recv()
        whole = slots[at, 0]
        for other in range(1, members(stages[at])):
            whole = whole + slots[at, other]
        own[at + 1] = whole

    def drain(name):
        for at in range(len(exchanges[name][0])):
            all_of(name, at).wait_send()

    def whole_exchange(name, first):
        stages = exchanges[name][0]
        for at in range(len(stages)):
            if at or not first:
                begin(name, at)
            finish(name, at)
        return exchanges[name][1][len(stages)] * (1.0 / count)

    def load_coefficients():
        @pl.loop(0, comp)
        def _(c):
            for d in range(coef.shape[0]):
                coef[d, c] = coef_in[d, c].astype(jnp.float32)
            for e in range(comp):
                for x in range(width):
                    edge_coef[c, e, x:x + 1, :] = coef[1, c, e, x, 0:1, :]
                    edge_coef[c, e, 4 + x:5 + x, :] = coef[2, c, e, x, ROWS - 1:ROWS, :]

        flat = comp * comp // 2
        for low in range(0, flat, 2):
            for side in (0, 1):
                both = []
                for at in (low, low + 1):
                    c, e = 2 * at // comp, 2 * at % comp
                    one, two = edge_coef[c, e], edge_coef[c, e + 1]
                    if side == 0:
                        both.append(jnp.where(low_rows, pltpu.roll(one, 4, 0), two))
                    else:
                        both.append(jnp.where(low_rows, one, pltpu.roll(two, 4, 0)))
                gz_send[side, ROWS * low:ROWS * (low + 2), :] = jnp.concatenate(
                    both, axis=0
                ).astype(jnp.bfloat16)

    def take_couplings():
        each_face(False, (0, 1), lambda kind, side: g_copy(kind, side).wait_recv())
        for low in range(0, comp * comp // 2, 2):
            below = gz_in[0, ROWS * low:ROWS * (low + 2), :].astype(jnp.float32)
            above = gz_in[1, ROWS * low:ROWS * (low + 2), :].astype(jnp.float32)
            for at in (0, 1):
                c, e = 2 * (low + at) // comp, 2 * (low + at) % comp
                b, a = below[ROWS * at:ROWS * (at + 1)], above[ROWS * at:ROWS * (at + 1)]
                gz[c, e] = split_pair(b, a, 0)
                gz[c, e + 1] = split_pair(b, a, 1)

    def complete_neighbours(r, step):
        for side, x in ((0, 0), (1, width - 1)):
            for c in range(comp):
                value = jnp.zeros((ROWS, LANES), jnp.float32)
                for e in range(comp):
                    value = value + gx_in[side, c, e].astype(jnp.float32) * allv[earlier + step, e, x]
                pre_x[side, c] = value
        total = jnp.zeros((comp, ROWS, LANES), jnp.float32)
        for e in range(comp):
            base = ROWS * (e // 2)
            own = split_pair(
                send_z[r, 0, 1, base:base + ROWS, :], send_z[r, 0, 0, base:base + ROWS, :], e % 2
            )
            total = total + gz[:, e] * own[None]
        pre_z[...] = total
        for sz in (0, 1):
            for sx in (0, 1):
                z = ROWS - 1 if sz == 0 else 0
                x = (4 if sz == 0 else 0) + (width - 1 if sx == 0 else 0)
                for c in range(comp):
                    send_c[r, sz, sx, c:c + 1, :] = pre_x[1 - sx, c, z:z + 1, :]
                    send_c[r, sz, sx, ROWS + c:ROWS + c + 1, :] = pre_z[c, x:x + 1, :]
        each_corner(True, lambda sz, sx: corner_copy(r, sz, sx).start())

    def take_ghosts(r, step):
        each_face(False, (1, 0), lambda kind, side: face_copy(r, step, 1, kind, side).wait_recv())
        each_corner(False, lambda sz, sx: corner_copy(r, sz, sx).wait_recv())
        for c in range(comp):
            value = pair_tile(halo_z, (r, 1), c) + pre_z[c]
            for sz in (0, 1):
                for sx in (0, 1):
                    row = (0 if sz == 0 else 4) + (0 if sx == 0 else width - 1)
                    value = value + jnp.where(row2 == row, halo_c[r, sz, sx, c:c + 1, :], 0.0)
            ghost_z[c] = value
            for side in (0, 1):
                value = halo_x[r, 1, side, c] + pre_x[side, c]
                for sz in (0, 1):
                    row = 0 if sz == 0 else ROWS - 1
                    value = value + jnp.where(
                        row2 == row, halo_c[r, sz, side, ROWS + c:ROWS + c + 1, :], 0.0
                    )
                ghost_x[side, c] = value

    with jax.named_scope("start"):
        copy_start.wait()
        wait_around(barrier, REACH, (1, 1))
        greet(0)

    step = 0
    comps = list(range(comp))
    paired = [r for r, size in enumerate(rounds) if size == 2]
    before = max(1, len(rounds) - 1)
    share = [2 * comp // (before + 1)] + [comp // (before + 1)] * (before - 1)
    share[-1] += comp - sum(share)
    share += [0] * (len(rounds) - len(share))
    greeted, ee_at, self_at, done = 1, None, 0, 0

    def self_some(low, high):
        @pl.loop(low, high)
        def _(c):
            self_products(c)

    for r, size in enumerate(rounds):
        with jax.named_scope(f"send{r}"):
            if r:
                each_face(
                    True, (0, 1), lambda kind, side: face_copy(r - 1, 0, 0, kind, side).wait_send()
                )
            send_faces(r, step)
        if r == 0:
            with jax.named_scope("load"):
                copy_coef.wait()
                load_coefficients()
                each_face(True, (0, 1), lambda kind, side: g_copy(kind, side).start())
                copy_shifts.wait()
        with jax.named_scope(f"neigh{r}"):
            if size == 2 and r == paired[0]:
                take_couplings()
            if size == 2:
                if r > paired[0]:
                    each_corner(True, lambda sz, sx: corner_copy(r - 1, sz, sx).wait_send())
                complete_neighbours(r, step)
        with jax.named_scope(f"local{r}"):
            part[r] = apply_local(step)
        with jax.named_scope(f"part{r}"):
            if size == 2:
                pack(r, 1, lambda e, x: part.at[r, e, x])
                if r > paired[0]:
                    each_face(
                        True, (0, 1),
                        lambda kind, side: face_copy(r - 1, 0, 1, kind, side).wait_send(),
                    )
                each_face(True, (0, 1), lambda kind, side: face_copy(r, step, 1, kind, side).start())
            if r == 0:
                copy_early.wait()
        with jax.named_scope(f"cross{r}"):
            for k in range(done, min(step + 1, late)):
                cross_products(k, sums_ref.at[k // 2], (k % 2) * half)
                done = k + 1
        with jax.named_scope(f"self{r}"):
            if share[r]:
                middle = self_at + share[r] // 2
                if r == 0:
                    self_some(self_at, middle)
                    greet(greeted)
                    greeted += 1
                    self_some(middle, self_at + share[r])
                else:
                    if greeted <= levels:
                        greet(greeted)
                        greeted += 1
                    self_some(self_at, self_at + share[r])
                self_at += share[r]
        with jax.named_scope(f"ee{r}"):
            if share[r] and self_at == comp:
                self_finish()
                while greeted <= levels:
                    greet(greeted)
                    greeted += 1
                begin("ee", 0)
                ee_at = 0
            elif ee_at == 0 and len(single) > 1:
                finish("ee", 0)
                begin("ee", 1)
                ee_at = 1
            if done == late and r == len(rounds) - 1:
                for q in range(lines):
                    mine_b[0, q] = as_line(sums_ref[q])
                begin("b", 0)
        with jax.named_scope(f"faces{r}"):
            take_faces(r, step, lambda x, r=r: part[r, :, x])
        if size == 2:
            with jax.named_scope(f"late{r}"):
                if r == len(rounds) - 1:
                    cross_products(step + 1, late_ref, 0)
            with jax.named_scope(f"second{r}"):
                acc_ref[...] = apply_local(step + 1)
            with jax.named_scope(f"ghost{r}"):
                take_ghosts(r, step)
            with jax.named_scope(f"store{r}"):
                sides = add_x(lambda x: acc_ref[:, x], lambda side, e: ghost_x[side, e])
                edge = add_z(lambda e: ghost_z[e])
                store_step(step + 2, lambda x: acc_ref[:, x], sides, edge)
        step += size

    with jax.named_scope("last"):
        cross_products(depth, late_ref, half)
        mine_f[0] = as_line(late_ref[...])
        begin("f", 0)

    with jax.named_scope("eewait"):
        for at in range(ee_at, len(single)):
            if at > ee_at:
                begin("ee", at)
            finish("ee", at)
        packed = mine_ee[len(single)] * (1.0 / count)
    with jax.named_scope("bwait"):
        early = whole_exchange("b", True)

    with jax.named_scope("algebra"):
        row, lane = iota((ROWS, LANES), 0), iota((ROWS, LANES), 1)
        found = jnp.concatenate(
            [
                early[k // 2] if k % 2 == 0 else pltpu.roll(early[k // 2], half, 1)
                for k in range(late)
            ] + [jnp.zeros((ROWS - late, LANES), jnp.float32)], axis=0
        )
        proj_t = jnp.where(lane < earlier, found, 0.0)
        known = jnp.where(lane < earlier + row, found, 0.0)
        pick = onehot((ROWS, LANES), lambda r, q: q == r + earlier)
        gram = jnp.where(lane <= earlier + row, found, 0.0)
        gram = pltpu.roll(gram, LANES - earlier, 1)[:, :ROWS]
        square = jnp.concatenate(
            [packed] + [pltpu.roll(packed, LANES - 32 * g, 1) for g in range(1, 4)], axis=0
        )
        sr, sl = iota(square.shape, 0), iota(square.shape, 1)
        inside = (sl < earlier) & (sr < earlier)
        square = jnp.where(inside, square - jnp.where(sr == sl, 2.0, 0.0), 0.0)
        moved = dot(proj_t[:, :32], square) + pick
        gram = gram + dot(moved, known, nt=True)

        upper = gram
        inverse = onehot((ROWS, ROWS), lambda r, q: (r == q) & (r < late))
        r8 = iota((ROWS, ROWS), 0)
        q8 = iota((ROWS, ROWS), 1)
        for p in range(late):
            pivot = upper[p:p + 1, p:p + 1]
            scale = inverse_root(pivot)
            column = upper[:, p:p + 1] * scale
            row_u, row_i = upper[p:p + 1, :] * scale, inverse[p:p + 1, :] * scale
            upper = jnp.where(r8 == p, row_u, jnp.where(r8 > p, upper - column * row_u, upper))
            inverse = jnp.where(r8 == p, row_i, jnp.where(r8 > p, inverse - column * row_i, inverse))
        onto = dot(inverse, moved)

        mix = dot(inverse, pick - proj_t)
        tall = dot(onehot((late * ROWS, ROWS), lambda r, q: (r >> 3) == q), mix)
        span = earlier * ROWS
        mix = split(diagonal(dot(tall, onehot((LANES, span), lambda r, q: (q >> 3) == r))))
        weights = [
            [
                jnp.broadcast_to(
                    tall[k * ROWS:(k + 1) * ROWS, earlier + i:earlier + i + 1], (ROWS, LANES)
                )
                for i in range(k + 1)
            ]
            for k in range(late)
        ]
    with jax.named_scope("out"):
        for c in range(comp):
            out = dot_pieces(mix, [pieces[at, c] for at in range(3)])
            for x in range(width):
                for k in range(late):
                    value = out[k * ROWS:(k + 1) * ROWS, LANES * x:LANES * (x + 1)]
                    for i in range(k + 1):
                        value = value + weights[k][i] * allv[earlier + i, c, x]
                    new_ref[k, c, x] = value
        small_ref[0:ROWS, :] = proj_t
        small_ref[ROWS:2 * ROWS, :] = jnp.zeros((ROWS, LANES), jnp.float32)
        small_ref[ROWS:2 * ROWS, 0:ROWS] = jnp.where((q8 >= r8) & (r8 < late), upper, 0.0)

    with jax.named_scope("sent"):
        r = len(rounds) - 1
        for what in range(2 if paired else 1):
            at = paired[-1] if what else r
            each_face(
                True, (0, 1), lambda kind, side: face_copy(at, 0, what, kind, side).wait_send()
            )
        if paired:
            each_corner(True, lambda sz, sx: corner_copy(paired[-1], sz, sx).wait_send())
        each_face(True, (0, 1), lambda kind, side: g_copy(kind, side).wait_send())
        drain("ee")
        drain("b")
    with jax.named_scope("fwait"):
        final = whole_exchange("f", True)
    with jax.named_scope("columns"):
        ys = [final, pltpu.roll(final, half, 1)][2 - (block - late):]
        spread = [jnp.broadcast_to(y, (ROWS, LANES)) for y in ys]
        tiles = -(-(earlier + block) // ROWS)
        columns = []
        for y in spread:
            col = [
                lane_sums(jnp.where(lane == row + ROWS * t, y, 0.0)) for t in range(tiles)
            ]
            img = [
                lane_sums(square[ROWS * t:ROWS * (t + 1)] * y) for t in range(square.shape[0] // ROWS)
            ]
            columns.append((col, img, lane_sums(onto * y)))
        wide = lambda value: jnp.broadcast_to(value, (ROWS, LANES))

        def inner(a, b):
            (col_a, _, r_a), (col_b, img_b, r_b) = columns[a], columns[b]
            total = -(r_a * r_b)
            for t in range(len(img_b)):
                total = total + jnp.where(row[:, :1] + ROWS * t < earlier, col_a[t] * img_b[t], 0.0)
            for t in range(tiles):
                total = total + jnp.where(row[:, :1] + ROWS * t == earlier + late + a, col_b[t], 0.0)
            return sublane_sums(wide(total))

        fresh = block - late
        scales, ratios, lines_out = [], {}, []
        for b in range(fresh):
            value = inner(b, b)
            for a in range(b):
                cross = inner(a, b)
                ratios[a, b] = cross * scales[a]
                value = value - ratios[a, b] * ratios[a, b]
            scales.append(inverse_root(value))
            ratios[b, b] = value * scales[b]
        triangle = small_ref[ROWS:2 * ROWS, :]
        proj_rows = small_ref[0:ROWS, :]
        for b in range(fresh):
            k = late + b
            triangle = triangle + jnp.where(lane == k, wide(columns[b][2]), 0.0)
            for a in range(b + 1):
                triangle = triangle + jnp.where((lane == k) & (row == late + a), ratios[a, b], 0.0)
            proj_rows = jnp.where((row == k) & (lane < earlier), spread[b], proj_rows)
        small_ref[ROWS:2 * ROWS, :] = triangle
        small_ref[0:ROWS, :] = proj_rows
        for b in range(fresh):
            for t in range(tiles):
                late_ref[b * half + ROWS * t:b * half + ROWS * (t + 1), :] = wide(columns[b][0][t])
            late_ref[b * half + ROWS * tiles:b * half + ROWS * (tiles + 1), :] = wide(columns[b][2])

    with jax.named_scope("tail"):
        for c in range(comp):
            totals = [allv[earlier + late + b, c] for b in range(fresh)]
            for j in range(earlier):
                v = allv[j, c]
                for b in range(fresh):
                    at = b * half + j
                    totals[b] = totals[b] - late_ref[at:at + 1, :] * v
            for i in range(late):
                v = new_ref[i, c]
                for b in range(fresh):
                    at = b * half + ROWS * tiles + i
                    totals[b] = totals[b] - late_ref[at:at + 1, :] * v
            outs = []
            for b in range(fresh):
                value = totals[b]
                for a in range(b):
                    value = value - ratios[a, b] * outs[a]
                outs.append(value * scales[b])
                new_ref[late + b, c] = outs[b]

    with jax.named_scope("drain"):
        drain("f")
        proj_ref[...] = small_ref[:block, :earlier]
        tri_ref[...] = small_ref[ROWS:ROWS + block, :block]


def hand_over(new_in, proj_in, tri_in, new_out, proj_out, tri_out, sem):
    pairs = ((new_in, new_out), (proj_in, proj_out), (tri_in, tri_out))
    copies = [pltpu.make_async_copy(*pair, sem.at[at]) for at, pair in enumerate(pairs)]
    for copy in copies:
        copy.start()
    for copy in copies:
        copy.wait()


def body(sizes, coefficients, earlier, start, shifts):
    coefficients = jnp.transpose(coefficients, (0, 1, 2, 4, 3, 5))
    earlier = jnp.transpose(earlier, (0, 1, 3, 2, 4))
    start = jnp.transpose(start, (0, 2, 1, 3))
    depth, count = shifts.shape[0], earlier.shape[0]
    block = depth + 1
    kinds, comp, _, width, rows, lanes = coefficients.shape
    rounds = len(steps_of(depth))
    late = block - steps_of(depth)[-1]
    lines = late // 2 + late % 2
    single, joint = stages_of(sizes), joint_stages_of(sizes)
    most = max(members(stage) for stage in single)
    joined = max(members(stage) for stage in joint)
    levels = max(1, levels_of([n for _, n in sizes]))
    f32, b16 = jnp.float32, jnp.bfloat16
    anywhere = pl.BlockSpec(memory_space=pl.ANY)
    vmem = pl.BlockSpec(memory_space=pltpu.VMEM)
    sems = pltpu.SemaphoreType.DMA
    found = pl.pallas_call(
        functools.partial(kernel, sizes),
        out_shape=(
            pltpu.VMEM((block, comp, width, rows, lanes), f32),
            pltpu.VMEM((block, count), f32),
            pltpu.VMEM((block, block), f32),
        ),
        in_specs=[anywhere] * 4,
        out_specs=(vmem, vmem, vmem),
        scratch_shapes=[
            pltpu.VMEM(coefficients.shape, coefficients.dtype),
            pltpu.VMEM(coefficients.shape, f32),
            pltpu.VMEM((comp, comp, rows, lanes), f32),
            pltpu.VMEM((2, comp, comp, rows, lanes), b16),
            pltpu.VMEM((2, 4 * comp * comp, lanes), b16),
            pltpu.VMEM((2, 4 * comp * comp, lanes), b16),
            pltpu.VMEM((comp, comp, rows, lanes), f32),
            pltpu.VMEM((count + block, comp, width, rows, lanes), f32),
            pltpu.VMEM((3, comp, count * rows, width * lanes), b16),
            pltpu.VMEM((rounds, comp, width, rows, lanes), f32),
            pltpu.VMEM((comp, width, rows, lanes), f32),
            pltpu.VMEM((rounds, 2, 2, comp, rows, lanes), f32),
            pltpu.VMEM((rounds, 2, 2, 4 * comp, lanes), f32),
            pltpu.VMEM((rounds, 2, 2, 4 * comp, lanes), f32),
            pltpu.VMEM((rounds, 2, 2, 2 * rows, lanes), f32),
            pltpu.VMEM((rounds, 2, 2, 2 * rows, lanes), f32),
            pltpu.VMEM((2, comp, rows, lanes), f32),
            pltpu.VMEM((comp, rows, lanes), f32),
            pltpu.VMEM((2, comp, rows, lanes), f32),
            pltpu.VMEM((comp, rows, lanes), f32),
            pltpu.VMEM((count * rows, count * rows), f32),
            pltpu.VMEM((count * rows, count * rows), f32),
            pltpu.VMEM((lines, lanes, lanes), f32),
            pltpu.VMEM((lanes, lanes), f32),
            pltpu.VMEM((2 * rows, lanes), f32),
            pltpu.VMEM((len(single) + 1, rows, lanes), f32),
            pltpu.VMEM((len(single), most, rows, lanes), f32),
            pltpu.VMEM((len(joint) + 1, lines, 1, lanes), f32),
            pltpu.VMEM((len(joint), joined, lines, 1, lanes), f32),
            pltpu.VMEM((len(joint) + 1, 1, lanes), f32),
            pltpu.VMEM((len(joint), joined, 1, lanes), f32),
            sems((4,)),
            sems((2, 2, 2)),
            sems((2, 2, 2, 2)),
            sems((2, 2)),
            sems((2, 2, 2)),
            sems((2, 2)),
            sems((2, 2)),
            sems((len(single),)),
            sems((len(single),)),
            sems((len(joint),)),
            sems((len(joint),)),
            sems((len(joint),)),
            sems((len(joint),)),
            pltpu.SemaphoreType.REGULAR((levels,)),
            pltpu.SMEM(shifts.shape, f32),
        ],
        compiler_params=pltpu.CompilerParams(collective_id=0, has_side_effects=True),
        name="powers",
    )(coefficients, earlier, start, shifts)
    found = [pltpu.with_memory_space_constraint(value, pltpu.VMEM) for value in found]
    new, proj, tri = pl.pallas_call(
        hand_over,
        out_shape=[jax.ShapeDtypeStruct(value.shape, f32) for value in found],
        in_specs=[vmem] * 3,
        out_specs=[anywhere] * 3,
        scratch_shapes=[sems((3,))],
        name="hand_over",
    )(*found)
    return jnp.transpose(new, (0, 1, 3, 2, 4)), proj.T, tri


def solution(mesh):
    sizes = (("slab", mesh.shape["slab"]), ("sub", mesh.shape["sub"]))
    placed = (
        P(None, None, None, "slab", "sub", None),
        P(None, None, "slab", "sub", None),
        P(None, "slab", "sub", None),
        P(),
    )
    return jax.shard_map(
        functools.partial(body, sizes),
        mesh=mesh,
        in_specs=placed,
        out_specs=(P(None, None, "slab", "sub", None), P(), P()),
        check_vma=False,
    )
```

```python
import functools

import jax
import jax.numpy as jnp
from jax import lax
from jax.experimental import pallas as pl
from jax.experimental.pallas import tpu as pltpu
from jax.sharding import PartitionSpec as P

MESH = pl.DeviceIdType.MESH
LANES = 128
ROWS = 8
REACH = (2, 1)


def dot(a, b, nt=False):
    return lax.dot_general(
        a, b, (((1,), (1 if nt else 0,)), ((), ())),
        precision=lax.Precision.HIGHEST, preferred_element_type=jnp.float32,
    )


def iota(shape, dim):
    return lax.broadcasted_iota(jnp.int32, shape, dim)


def onehot(shape, test):
    return jnp.where(test(iota(shape, 0), iota(shape, 1)), 1.0, 0.0).astype(jnp.float32)


def diagonal(value):
    r, q = iota(value.shape, 0), iota(value.shape, 1)
    return jnp.where((r & 7) == (q & 7), value, 0.0)


def split(value):
    first = value.astype(jnp.bfloat16)
    left = value - first.astype(jnp.float32)
    second = left.astype(jnp.bfloat16)
    third = (left - second.astype(jnp.float32)).astype(jnp.bfloat16)
    return [first, second, third]


def dot_pieces(a, b, nt=False):
    found = None
    rows = a[0].shape[0]
    for at in (2, 1, 0):
        left = jnp.concatenate(a[: 3 - at], axis=0)
        part = lax.dot_general(
            left, b[at], (((1,), (1 if nt else 0,)), ((), ())),
            preferred_element_type=jnp.float32,
        )
        for i in reversed(range(3 - at)):
            piece = part[i * rows:(i + 1) * rows]
            found = piece if found is None else found + piece
    return found


def side_by_side(value):
    count, width = value.shape[0], value.shape[1]
    return jnp.concatenate(
        [value[:, x].reshape(count * ROWS, LANES) for x in range(width)], axis=1
    )


def factors(count):
    found = []
    while count > 1:
        fits = [f for f in range(2, min(count, 8) + 1) if count % f == 0]
        found.append(max(fits) if fits else count)
        count //= found[-1]
    return found


def stages_of(sizes):
    found = []
    for at, (_, count) in enumerate(sizes):
        stride = 1
        for size in factors(count):
            found.append(((stride, size), (1, 1)) if at == 0 else ((1, 1), (stride, size)))
            stride *= size
    return found


def joint_stages_of(sizes):
    slabs, subs = stages_of(sizes[:1]), [s[1] for s in stages_of((("", 1), sizes[1]))]
    first = slabs[0][0] if slabs else (1, 1)
    found = [(first, subs[0] if subs else (1, 1))]
    found += [(s[0], (1, 1)) for s in slabs[1:]] + [((1, 1), s) for s in subs[1:]]
    return found


def levels_of(extent):
    levels = 0
    while any(reach << levels < n - 1 for reach, n in zip(REACH, extent)):
        levels += 1
    return levels


def members(stage):
    return stage[0][1] * stage[1][1]


def offsets_of(stage):
    return [(a, b) for a in range(stage[0][1]) for b in range(stage[1][1]) if a or b]


def steps_of(depth):
    return ([1] if depth % 2 else []) + [2] * (depth // 2)


def lane_sums(value):
    return jnp.sum(value, axis=1, keepdims=True)


def sublane_sums(value):
    for shift in (4, 2, 1):
        value = value + pltpu.roll(value, shift, 0)
    return value


def inverse_root(value):
    scale = lax.rsqrt(value)
    return scale * (1.5 - 0.5 * value * scale * scale)


def kernel(
    sizes, coef_hbm, early_hbm, start_hbm, shifts_hbm, new_ref, proj_ref, tri_ref,
    coef_in, coef, edge_coef, gx_in, gz_send, gz_in, gz, allv, pieces, part, acc_ref,
    halo_x, halo_z, send_z, send_c, halo_c, pre_x, pre_z, ghost_x, ghost_z,
    ee, ee_cross, sums_ref, late_ref, small_ref, change_ref,
    mine_ee, gathered_ee, mine_b, gathered_b, mine_f, gathered_f,
    in_sem, face_send, face_recv, corner_send, corner_recv, g_send, g_recv,
    ee_send, ee_recv, b_send, b_recv, f_send, f_recv, ready, shifts_ref,
):
    depth = shifts_ref.shape[0]
    earlier, comp, width = early_hbm.shape[:3]
    block = depth + 1
    count = comp * width * ROWS * LANES * sizes[0][1] * sizes[1][1]
    half = LANES // 2
    rounds = steps_of(depth)
    single = stages_of(sizes)[::-1]
    joint = joint_stages_of(sizes)
    place = [lax.axis_index(axis) for axis, _ in sizes]
    extent = [n for _, n in sizes]
    names = [axis for axis, _ in sizes]
    late = block - rounds[-1]
    lines = late // 2 + late % 2

    copy_start = pltpu.make_async_copy(start_hbm, allv.at[earlier], in_sem.at[0])
    def coef_part(low, high, sem):
        part = pl.ds(low, high - low)
        return pltpu.make_async_copy(coef_hbm.at[part], coef_in.at[part], in_sem.at[sem])

    kinds = coef_hbm.shape[0]
    copy_height, copy_rest = coef_part(1, 3, 1), [coef_part(3, kinds, 4), coef_part(0, 1, 5)]
    copy_early = pltpu.make_async_copy(early_hbm, allv.at[pl.ds(0, earlier)], in_sem.at[2])
    copy_shifts = pltpu.make_async_copy(shifts_hbm, shifts_ref, in_sem.at[3])
    copy_start.start()
    copy_shifts.start()
    copy_height.start()
    for copy in copy_rest:
        copy.start()

    def there(kind, side, sending):
        upward = (side == 0) == sending
        return place[kind] < extent[kind] - 1 if upward else place[kind] > 0

    def at_peer(dz, dx):
        return {names[0]: place[0] + dz, names[1]: place[1] + dx}

    def toward(side):
        return 1 if side == 0 else -1

    def peer(stage, offset):
        mine_at, peer_at, target = [], [], {}
        for axis in (0, 1):
            stride, size = stage[axis]
            digit = lax.rem(place[axis] // stride, size)
            other = lax.rem(digit + offset[axis], size)
            mine_at.append(digit)
            peer_at.append(other)
            target[names[axis]] = place[axis] + (other - digit) * stride
        flat = stage[1][1]
        return mine_at[0] * flat + mine_at[1], peer_at[0] * flat + peer_at[1], target

    levels = levels_of(extent)

    def around(reach, unit, act):
        for dz in range(-reach[0], reach[0] + 1):
            for dx in range(-reach[1], reach[1] + 1):
                far = (unit[0] * dz, unit[1] * dx)
                if far != (0, 0):
                    a, b = place[0] + far[0], place[1] + far[1]

                    @pl.when((a >= 0) & (a < extent[0]) & (b >= 0) & (b < extent[1]))
                    def _():
                        act(at_peer(*far))

    def signal(sem):
        return lambda where: pl.semaphore_signal(
            sem, inc=1, device_id=where, device_id_type=MESH
        )

    def wait_around(sem, reach, unit):
        total = 1
        for axis in (0, 1):
            seen = 1
            for d in range(1, reach[axis] + 1):
                far = d * unit[axis]
                seen = seen + jnp.where(place[axis] >= far, 1, 0)
                seen = seen + jnp.where(place[axis] + far < extent[axis], 1, 0)
            total = total * seen
        pl.semaphore_wait(sem, total - 1)

    def greet(level):
        if 0 < level <= levels:
            unit = tuple(x << (level - 1) for x in REACH)
            wait_around(ready.at[level - 1], (1, 1), unit)
        if level < levels:
            unit = tuple(x << level for x in REACH)
            around((1, 1), unit, signal(ready.at[level]))

    barrier = pltpu.get_barrier_semaphore()
    around(REACH, (1, 1), signal(barrier))

    for kind in (0, 1):
        for side in (0, 1):
            @pl.when(jnp.logical_not(there(kind, side, False)))
            def _():
                halo, coupling = (halo_z, gz_in) if kind == 0 else (halo_x, gx_in)
                for r in range(len(rounds)):
                    for what in (0, 1):
                        halo[r, what, side] = jnp.zeros_like(halo[r, what, side])
                coupling[side] = jnp.zeros_like(coupling[side])
    for sz in (0, 1):
        for sx in (0, 1):
            @pl.when(jnp.logical_not(there(0, sz, False) & there(1, sx, False)))
            def _():
                for r in range(len(rounds)):
                    halo_c[r, sz, sx] = jnp.zeros_like(halo_c[r, sz, sx])

    send_z[...] = jnp.zeros_like(send_z)
    send_c[...] = jnp.zeros_like(send_c)
    edge_coef[...] = jnp.zeros_like(edge_coef)
    ee[...] = jnp.zeros_like(ee)
    ee_cross[...] = jnp.zeros_like(ee_cross)
    sums_ref[...] = jnp.zeros_like(sums_ref)
    late_ref[...] = jnp.zeros_like(late_ref)

    def face_copy(r, step, what, kind, side):
        if kind == 0:
            src, dst = send_z.at[r, what, side], halo_z.at[r, what, side]
        else:
            x = width - 1 if side == 0 else 0
            src = allv.at[earlier + step, :, x] if what == 0 else part.at[r, :, x]
            dst = halo_x.at[r, what, side]
        dz, dx = (toward(side), 0) if kind == 0 else (0, toward(side))
        return pltpu.make_async_remote_copy(
            src_ref=src, dst_ref=dst,
            send_sem=face_send.at[what, kind, side],
            recv_sem=face_recv.at[r % 2, what, kind, side],
            device_id=at_peer(dz, dx), device_id_type=MESH,
        )

    def corner_copy(r, sz, sx):
        return pltpu.make_async_remote_copy(
            src_ref=send_c.at[r, sz, sx], dst_ref=halo_c.at[r, sz, sx],
            send_sem=corner_send.at[sz, sx], recv_sem=corner_recv.at[r % 2, sz, sx],
            device_id=at_peer(toward(sz), toward(sx)), device_id_type=MESH,
        )

    def g_copy(kind, side):
        if kind == 0:
            src, dst = gz_send.at[side], gz_in.at[side]
        else:
            src = coef_in.at[4, :, :, width - 1] if side == 0 else coef_in.at[3, :, :, 0]
            dst = gx_in.at[side]
        dz, dx = (toward(side), 0) if kind == 0 else (0, toward(side))
        return pltpu.make_async_remote_copy(
            src_ref=src, dst_ref=dst, send_sem=g_send.at[kind, side],
            recv_sem=g_recv.at[kind, side], device_id=at_peer(dz, dx), device_id_type=MESH,
        )

    def each_face(sending, kinds, act):
        for kind in kinds:
            for side in (0, 1):
                @pl.when(there(kind, side, sending))
                def _():
                    act(kind, side)

    def each_corner(sending, act):
        for sz in (0, 1):
            for sx in (0, 1):
                @pl.when(there(0, sz, sending) & there(1, sx, sending))
                def _():
                    act(sz, sx)

    def pack(r, what, source):
        for e in range(comp):
            for x in range(width):
                row = 4 * e + x
                tile = source(e, x)
                send_z[r, what, 0, row:row + 1, :] = tile[ROWS - 1:ROWS, :]
                send_z[r, what, 1, row:row + 1, :] = tile[0:1, :]

    def send_faces(r, step):
        pack(r, 0, lambda e, x: allv.at[earlier + step, e, x])
        each_face(True, (0, 1), lambda kind, side: face_copy(r, step, 0, kind, side).start())

    row2 = iota((ROWS, LANES), 0)
    row3 = iota((width, ROWS, LANES), 1)
    lane3 = iota((width, ROWS, LANES), 2)
    zero_tile = jnp.zeros((1, ROWS, LANES), jnp.float32)
    low_rows = row2 < 4

    def split_pair(below, above, odd):
        if odd:
            return jnp.where(low_rows, pltpu.roll(below, 4, 0), above)
        return jnp.where(low_rows, below, pltpu.roll(above, 4, 0))

    def pair_tile(ref, index, e):
        base = ROWS * (e // 2)
        return split_pair(
            ref[(*index, 0, slice(base, base + ROWS))],
            ref[(*index, 1, slice(base, base + ROWS))], e % 2,
        )

    def apply_local(step):
        acc = 0.0
        for e in range(comp):
            v = allv[earlier + step, e]
            near = [
                v,
                jnp.where(row3 > 0, pltpu.roll(v, 1, 1), 0.0),
                jnp.where(row3 < ROWS - 1, pltpu.roll(v, ROWS - 1, 1), 0.0),
                jnp.concatenate([zero_tile, v[:-1]], axis=0),
                jnp.concatenate([v[1:], zero_tile], axis=0),
                jnp.where(lane3 > 0, pltpu.roll(v, 1, 2), 0.0),
                jnp.where(lane3 < LANES - 1, pltpu.roll(v, LANES - 1, 2), 0.0),
            ]
            for d in range(len(near)):
                acc = acc + coef[d, :, e] * near[d][None]
        return acc

    def add_x(source, x_of):
        found = []
        for side, d, x in ((0, 3, 0), (1, 4, width - 1)):
            value = source(x)
            for e in range(comp):
                value = value + coef[d, :, e, x] * x_of(side, e)[None]
            found.append(value)
        return found

    def add_z(z_of):
        edge = jnp.zeros((comp, ROWS, LANES), jnp.float32)
        for e in range(comp):
            edge = edge + edge_coef[:, e] * z_of(e)[None]
        return edge

    def store_step(step, source, sides, edge):
        for c in range(comp):
            for x in range(width):
                value = sides[0][c] if x == 0 else sides[1][c] if x == width - 1 else source(x)[c]
                value = value + jnp.where(
                    row2 == 0, edge[c, x:x + 1, :],
                    jnp.where(row2 == ROWS - 1, edge[c, 4 + x:5 + x, :], 0.0),
                )
                allv[earlier + step, c, x] = value

    def take_faces(r, step, source):
        each_face(False, (1,), lambda kind, side: face_copy(r, step, 0, kind, side).wait_recv())
        sides = add_x(source, lambda side, e: halo_x[r, 0, side, e])
        each_face(False, (0,), lambda kind, side: face_copy(r, step, 0, kind, side).wait_recv())
        edge = add_z(lambda e: pair_tile(halo_z, (r, 0), e))
        store_step(step + 1, source, sides, edge)

    def cross_products(k, ref, base):
        total, group = earlier + k + 1, 6
        w = allv[earlier + k]
        for low in range(0, total, group):
            high = min(low + group, total)
            sums = jnp.sum(w[None] * allv[low:high], axis=(1, 2))
            ref[base + low:base + high, :] = jnp.sum(sums, axis=1)

    def as_line(value):
        return jnp.sum(value.T, axis=0, keepdims=True)

    def times(a, b):
        return lax.dot_general(
            a, b, (((1,), (1,)), ((), ())), preferred_element_type=jnp.float32
        )

    def self_products(c):
        parts = split(side_by_side(allv[pl.ds(0, earlier), c]))
        for at, piece in enumerate(parts):
            pieces[at, c] = piece
        one = times(parts[0], parts[0])
        two = times(jnp.concatenate(parts[:2], axis=0), parts[1])
        three = times(parts[0], parts[2])
        span = earlier * ROWS
        ee[...] += one + two[span:]
        ee_cross[...] += two[:span] + three

    def gather_self(value):
        span = earlier * ROWS
        rows = jnp.sum(diagonal(value).reshape(earlier, ROWS, span), axis=1)
        own = onehot((span, LANES), lambda r, q: (r >> 3) == q).astype(jnp.bfloat16)
        found = None
        for piece in split(rows)[::-1]:
            some = lax.dot_general(
                piece, own, (((1,), (0,)), ((), ())), preferred_element_type=jnp.float32
            )
            found = some if found is None else found + some
        return jnp.concatenate(
            [found, jnp.zeros((LANES - earlier, LANES), jnp.float32)], axis=0
        )

    def self_finish():
        cross = gather_self(ee_cross[...])
        whole = gather_self(ee[...])[:32] + (cross + cross.T)[:32]
        packed = whole[:ROWS]
        for g in range(1, 4):
            packed = packed + pltpu.roll(whole[ROWS * g:ROWS * (g + 1)], 32 * g, 1)
        mine_ee[0, :ROWS] = packed
        mine_ee[0, ROWS:] = as_line(sums_ref[0])

    exchanges = {
        "ee": (single, mine_ee, gathered_ee, ee_send, ee_recv),
        "b": (joint, mine_b, gathered_b, b_send, b_recv),
        "f": (joint, mine_f, gathered_f, f_send, f_recv),
    }

    def begin(name, at):
        stages, own, slots, send_sem, recv_sem = exchanges[name]
        for offset in offsets_of(stages[at]):
            here, _, target = peer(stages[at], offset)
            pltpu.make_async_remote_copy(
                src_ref=own.at[at], dst_ref=slots.at[at, here],
                send_sem=send_sem.at[at], recv_sem=recv_sem.at[at],
                device_id=target, device_id_type=MESH,
            ).start()

    def all_of(name, at):
        stages, own, slots, send_sem, recv_sem = exchanges[name]
        others = slots.at[at, pl.ds(0, members(stages[at]) - 1)]
        _, _, target = peer(stages[at], offsets_of(stages[at])[0])
        return pltpu.make_async_remote_copy(
            src_ref=others, dst_ref=others, send_sem=send_sem.at[at], recv_sem=recv_sem.at[at],
            device_id=target, device_id_type=MESH,
        )

    def finish(name, at):
        stages, own, slots, _, _ = exchanges[name]
        here, _, _ = peer(stages[at], (0, 0))
        slots[at, here] = own[at]
        all_of(name, at).wait_recv()
        whole = slots[at, 0]
        for other in range(1, members(stages[at])):
            whole = whole + slots[at, other]
        own[at + 1] = whole

    def drain(name):
        for at in range(len(exchanges[name][0])):
            all_of(name, at).wait_send()

    def whole_exchange(name, first):
        stages = exchanges[name][0]
        for at in range(len(stages)):
            if at or not first:
                begin(name, at)
            finish(name, at)
        return exchanges[name][1][len(stages)] * (1.0 / count)

    def load_height():
        @pl.loop(0, comp)
        def _(c):
            for d in (1, 2):
                coef[d, c] = coef_in[d, c].astype(jnp.float32)
            for e in range(comp):
                for x in range(width):
                    edge_coef[c, e, x:x + 1, :] = coef[1, c, e, x, 0:1, :]
                    edge_coef[c, e, 4 + x:5 + x, :] = coef[2, c, e, x, ROWS - 1:ROWS, :]

        flat = comp * comp // 2
        for low in range(0, flat, 2):
            for side in (0, 1):
                both = []
                for at in (low, low + 1):
                    c, e = 2 * at // comp, 2 * at % comp
                    one, two = edge_coef[c, e], edge_coef[c, e + 1]
                    if side == 0:
                        both.append(jnp.where(low_rows, pltpu.roll(one, 4, 0), two))
                    else:
                        both.append(jnp.where(low_rows, one, pltpu.roll(two, 4, 0)))
                gz_send[side, ROWS * low:ROWS * (low + 2), :] = jnp.concatenate(
                    both, axis=0
                ).astype(jnp.bfloat16)

    def load_rest():
        @pl.loop(0, comp)
        def _(c):
            for d in (0, *range(3, coef.shape[0])):
                coef[d, c] = coef_in[d, c].astype(jnp.float32)

    def take_couplings():
        each_face(False, (0, 1), lambda kind, side: g_copy(kind, side).wait_recv())
        for low in range(0, comp * comp // 2, 2):
            below = gz_in[0, ROWS * low:ROWS * (low + 2), :].astype(jnp.float32)
            above = gz_in[1, ROWS * low:ROWS * (low + 2), :].astype(jnp.float32)
            for at in (0, 1):
                c, e = 2 * (low + at) // comp, 2 * (low + at) % comp
                b, a = below[ROWS * at:ROWS * (at + 1)], above[ROWS * at:ROWS * (at + 1)]
                gz[c, e] = split_pair(b, a, 0)
                gz[c, e + 1] = split_pair(b, a, 1)

    def complete_neighbours(r, step):
        for side, x in ((0, 0), (1, width - 1)):
            for c in range(comp):
                value = jnp.zeros((ROWS, LANES), jnp.float32)
                for e in range(comp):
                    value = value + gx_in[side, c, e].astype(jnp.float32) * allv[earlier + step, e, x]
                pre_x[side, c] = value
        total = jnp.zeros((comp, ROWS, LANES), jnp.float32)
        for e in range(comp):
            base = ROWS * (e // 2)
            own = split_pair(
                send_z[r, 0, 1, base:base + ROWS, :], send_z[r, 0, 0, base:base + ROWS, :], e % 2
            )
            total = total + gz[:, e] * own[None]
        pre_z[...] = total
        for sz in (0, 1):
            for sx in (0, 1):
                z = ROWS - 1 if sz == 0 else 0
                x = (4 if sz == 0 else 0) + (width - 1 if sx == 0 else 0)
                for c in range(comp):
                    send_c[r, sz, sx, c:c + 1, :] = pre_x[1 - sx, c, z:z + 1, :]
                    send_c[r, sz, sx, ROWS + c:ROWS + c + 1, :] = pre_z[c, x:x + 1, :]
        each_corner(True, lambda sz, sx: corner_copy(r, sz, sx).start())

    def take_ghosts(r, step):
        each_face(False, (1, 0), lambda kind, side: face_copy(r, step, 1, kind, side).wait_recv())
        each_corner(False, lambda sz, sx: corner_copy(r, sz, sx).wait_recv())
        for c in range(comp):
            value = pair_tile(halo_z, (r, 1), c) + pre_z[c]
            for sz in (0, 1):
                for sx in (0, 1):
                    row = (0 if sz == 0 else 4) + (0 if sx == 0 else width - 1)
                    value = value + jnp.where(row2 == row, halo_c[r, sz, sx, c:c + 1, :], 0.0)
            ghost_z[c] = value
            for side in (0, 1):
                value = halo_x[r, 1, side, c] + pre_x[side, c]
                for sz in (0, 1):
                    row = 0 if sz == 0 else ROWS - 1
                    value = value + jnp.where(
                        row2 == row, halo_c[r, sz, side, ROWS + c:ROWS + c + 1, :], 0.0
                    )
                ghost_x[side, c] = value

    with jax.named_scope("start"):
        copy_start.wait()
        copy_early.start()
        wait_around(barrier, REACH, (1, 1))
        greet(0)

    step = 0
    comps = list(range(comp))
    paired = [r for r, size in enumerate(rounds) if size == 2]
    before = max(1, len(rounds) - 1)
    share = [2 * comp // (before + 1)] + [comp // (before + 1)] * (before - 1)
    share[-1] += comp - sum(share)
    share += [0] * (len(rounds) - len(share))
    greeted, ee_at, self_at, done = 1, None, 0, 0

    def self_some(low, high):
        @pl.loop(low, high)
        def _(c):
            self_products(c)

    for r, size in enumerate(rounds):
        with jax.named_scope(f"send{r}"):
            if r:
                each_face(
                    True, (0, 1), lambda kind, side: face_copy(r - 1, 0, 0, kind, side).wait_send()
                )
            send_faces(r, step)
        if r == 0:
            with jax.named_scope("load"):
                copy_height.wait()
                load_height()
                each_face(True, (0,), lambda kind, side: g_copy(kind, side).start())
                for copy in copy_rest:
                    copy.wait()
                each_face(True, (1,), lambda kind, side: g_copy(kind, side).start())
                load_rest()
        with jax.named_scope(f"local{r}"):
            part[r] = apply_local(step)
        with jax.named_scope(f"part{r}"):
            if size == 2:
                pack(r, 1, lambda e, x: part.at[r, e, x])
                if r > paired[0]:
                    each_face(
                        True, (0, 1),
                        lambda kind, side: face_copy(r - 1, 0, 1, kind, side).wait_send(),
                    )
                each_face(True, (0, 1), lambda kind, side: face_copy(r, step, 1, kind, side).start())
        with jax.named_scope(f"neigh{r}"):
            if size == 2 and r == paired[0]:
                take_couplings()
            if size == 2:
                if r > paired[0]:
                    each_corner(True, lambda sz, sx: corner_copy(r - 1, sz, sx).wait_send())
                complete_neighbours(r, step)
        with jax.named_scope(f"cross{r}"):
            if len(rounds) == 1:
                copy_early.wait()
            if r or len(rounds) == 1:
                for k in range(done, min(step + 1, late)):
                    cross_products(k, sums_ref.at[k // 2], (k % 2) * half)
                    done = k + 1
        with jax.named_scope(f"self{r}"):
            if share[r]:
                middle = self_at + share[r] // 2
                if r == 0:
                    if len(rounds) > 1:
                        copy_early.wait()
                    self_some(self_at, middle)
                    greet(greeted)
                    greeted += 1
                    self_some(middle, self_at + share[r])
                else:
                    if greeted <= levels:
                        greet(greeted)
                        greeted += 1
                    self_some(self_at, self_at + share[r])
                self_at += share[r]
        with jax.named_scope(f"ee{r}"):
            if done == late and r == len(rounds) - 1:
                for q in range(1, lines):
                    mine_b[0, q - 1] = as_line(sums_ref[q])
                begin("b", 0)
            if share[r] and self_at == comp:
                self_finish()
                while greeted <= levels:
                    greet(greeted)
                    greeted += 1
                begin("ee", 0)
                ee_at = 0
            elif ee_at == 0 and len(single) > 1:
                finish("ee", 0)
                begin("ee", 1)
                ee_at = 1
        with jax.named_scope(f"faces{r}"):
            take_faces(r, step, lambda x, r=r: part[r, :, x])
        if size == 2:
            with jax.named_scope(f"late{r}"):
                if r == len(rounds) - 1:
                    cross_products(step + 1, late_ref, 0)
            with jax.named_scope(f"second{r}"):
                acc_ref[...] = apply_local(step + 1)
            with jax.named_scope(f"ghost{r}"):
                take_ghosts(r, step)
            with jax.named_scope(f"store{r}"):
                sides = add_x(lambda x: acc_ref[:, x], lambda side, e: ghost_x[side, e])
                edge = add_z(lambda e: ghost_z[e])
                store_step(step + 2, lambda x: acc_ref[:, x], sides, edge)
        step += size

    with jax.named_scope("last"):
        cross_products(depth, late_ref, half)
        mine_f[0] = as_line(late_ref[...])
        begin("f", 0)

    with jax.named_scope("eewait"):
        for at in range(ee_at, len(single)):
            if at > ee_at:
                begin("ee", at)
            finish("ee", at)
        packed = mine_ee[len(single), :ROWS] * (1.0 / count)
        ahead = mine_ee[len(single), ROWS:] * (1.0 / count)
    row, lane = iota((ROWS, LANES), 0), iota((ROWS, LANES), 1)
    with jax.named_scope("change"):
        copy_shifts.wait()
        unit, nothing = jnp.ones((ROWS, LANES), jnp.float32), jnp.zeros((ROWS, LANES), jnp.float32)
        change = [[unit]]
        for k in range(depth):
            last, scale = change[-1], 1.0 - shifts_ref[k]
            change.append(
                [
                    (last[m - 1] if m else nothing) + (scale * last[m] if m <= k else nothing)
                    for m in range(k + 2)
                ]
            )
        for m in range(block):
            down, along = nothing, nothing
            for k in range(m, block):
                down = jnp.where(row == k, change[k][m], down)
                along = jnp.where(lane == k, change[k][m], along)
            change_ref[0, m] = down
            change_ref[1, m] = along
    with jax.named_scope("bwait"):
        early = whole_exchange("b", True)

    with jax.named_scope("algebra"):
        found = jnp.concatenate(
            [
                pltpu.roll(ahead if k < 2 else early[k // 2 - 1], (k % 2) * half, 1)
                for k in range(late)
            ] + [jnp.zeros((ROWS - late, LANES), jnp.float32)], axis=0
        )
        proj_t = jnp.where(lane < earlier, found, 0.0)
        known = jnp.where(lane < earlier + row, found, 0.0)
        pick = onehot((ROWS, LANES), lambda r, q: q == r + earlier)
        gram = jnp.where(lane <= earlier + row, found, 0.0)
        gram = pltpu.roll(gram, LANES - earlier, 1)[:, :ROWS]
        square = jnp.concatenate(
            [packed] + [pltpu.roll(packed, LANES - 32 * g, 1) for g in range(1, 4)], axis=0
        )
        sr, sl = iota(square.shape, 0), iota(square.shape, 1)
        inside = (sl < earlier) & (sr < earlier)
        square = jnp.where(inside, square - jnp.where(sr == sl, 2.0, 0.0), 0.0)
        moved = dot(proj_t[:, :32], square) + pick
        gram = gram + dot(moved, known, nt=True)

        upper = gram
        inverse = onehot((ROWS, ROWS), lambda r, q: (r == q) & (r < late))
        r8 = iota((ROWS, ROWS), 0)
        q8 = iota((ROWS, ROWS), 1)
        for p in range(late):
            pivot = upper[p:p + 1, p:p + 1]
            scale = inverse_root(pivot)
            column = upper[:, p:p + 1] * scale
            row_u, row_i = upper[p:p + 1, :] * scale, inverse[p:p + 1, :] * scale
            upper = jnp.where(r8 == p, row_u, jnp.where(r8 > p, upper - column * row_u, upper))
            inverse = jnp.where(r8 == p, row_i, jnp.where(r8 > p, inverse - column * row_i, inverse))
        onto = dot(inverse, moved)

        mix = dot(inverse, pick - proj_t)
        tall = jnp.concatenate(
            [jnp.broadcast_to(mix[k:k + 1], (ROWS, LANES)) for k in range(late)], axis=0
        )
        span = earlier * ROWS
        grow = onehot((LANES, span), lambda r, q: (q >> 3) == r).astype(jnp.bfloat16)
        mix = [
            diagonal(
                lax.dot_general(
                    piece, grow, (((1,), (0,)), ((), ())), preferred_element_type=jnp.float32
                )
            ).astype(jnp.bfloat16)
            for piece in split(tall)
        ]
        weights = [
            [
                jnp.broadcast_to(
                    tall[k * ROWS:(k + 1) * ROWS, earlier + i:earlier + i + 1], (ROWS, LANES)
                )
                for i in range(k + 1)
            ]
            for k in range(late)
        ]
    with jax.named_scope("out"):
        for c in range(comp):
            out = dot_pieces(mix, [pieces[at, c] for at in range(3)])
            for x in range(width):
                for k in range(late):
                    value = out[k * ROWS:(k + 1) * ROWS, LANES * x:LANES * (x + 1)]
                    for i in range(k + 1):
                        value = value + weights[k][i] * allv[earlier + i, c, x]
                    new_ref[k, c, x] = value
        proj_early, tri_early = 0.0, 0.0
        for m in range(late):
            proj_early = proj_early + change_ref[0, m] * proj_t[m:m + 1]
            column = jnp.where(r8[:, :1] <= m, upper[:, m:m + 1], 0.0)
            tri_early = tri_early + change_ref[1, m] * column
        small_ref[0:ROWS, :] = proj_early
        small_ref[ROWS:2 * ROWS, :] = jnp.where(row < late, tri_early, 0.0)

    with jax.named_scope("sent"):
        r = len(rounds) - 1
        for what in range(2 if paired else 1):
            at = paired[-1] if what else r
            each_face(
                True, (0, 1), lambda kind, side: face_copy(at, 0, what, kind, side).wait_send()
            )
        if paired:
            each_corner(True, lambda sz, sx: corner_copy(paired[-1], sz, sx).wait_send())
        each_face(True, (0, 1), lambda kind, side: g_copy(kind, side).wait_send())
        drain("ee")
        drain("b")
    with jax.named_scope("fwait"):
        final = whole_exchange("f", True)
    with jax.named_scope("columns"):
        ys = [final, pltpu.roll(final, half, 1)][2 - (block - late):]
        spread = [jnp.broadcast_to(y, (ROWS, LANES)) for y in ys]
        tiles = -(-(earlier + block) // ROWS)
        columns = []
        for y in spread:
            col = [
                lane_sums(jnp.where(lane == row + ROWS * t, y, 0.0)) for t in range(tiles)
            ]
            img = [
                lane_sums(square[ROWS * t:ROWS * (t + 1)] * y) for t in range(square.shape[0] // ROWS)
            ]
            columns.append((col, img, lane_sums(onto * y)))
        wide = lambda value: jnp.broadcast_to(value, (ROWS, LANES))

        def inner(a, b):
            (col_a, _, r_a), (col_b, img_b, r_b) = columns[a], columns[b]
            total = -(r_a * r_b)
            for t in range(len(img_b)):
                total = total + jnp.where(row[:, :1] + ROWS * t < earlier, col_a[t] * img_b[t], 0.0)
            for t in range(tiles):
                total = total + jnp.where(row[:, :1] + ROWS * t == earlier + late + a, col_b[t], 0.0)
            return sublane_sums(wide(total))

        fresh = block - late
        scales, ratios, lines_out = [], {}, []
        for b in range(fresh):
            value = inner(b, b)
            for a in range(b):
                cross = inner(a, b)
                ratios[a, b] = cross * scales[a]
                value = value - ratios[a, b] * ratios[a, b]
            scales.append(inverse_root(value))
            ratios[b, b] = value * scales[b]
        triangle = small_ref[ROWS:2 * ROWS, :]
        proj_rows = small_ref[0:ROWS, :]
        for b in range(fresh):
            column = wide(columns[b][2])
            for a in range(b + 1):
                column = jnp.where(row == late + a, ratios[a, b], column)
            triangle = triangle + change_ref[1, late + b] * column
            proj_rows = proj_rows + change_ref[0, late + b] * spread[b]
        small_ref[ROWS:2 * ROWS, :] = triangle
        small_ref[0:ROWS, :] = proj_rows
        for b in range(fresh):
            for t in range(tiles):
                late_ref[b * half + ROWS * t:b * half + ROWS * (t + 1), :] = wide(columns[b][0][t])
            late_ref[b * half + ROWS * tiles:b * half + ROWS * (tiles + 1), :] = wide(columns[b][2])

    with jax.named_scope("tail"):
        for c in range(comp):
            totals = [allv[earlier + late + b, c] for b in range(fresh)]
            for j in range(earlier):
                v = allv[j, c]
                for b in range(fresh):
                    at = b * half + j
                    totals[b] = totals[b] - late_ref[at:at + 1, :] * v
            for i in range(late):
                v = new_ref[i, c]
                for b in range(fresh):
                    at = b * half + ROWS * tiles + i
                    totals[b] = totals[b] - late_ref[at:at + 1, :] * v
            outs = []
            for b in range(fresh):
                value = totals[b]
                for a in range(b):
                    value = value - ratios[a, b] * outs[a]
                outs.append(value * scales[b])
                new_ref[late + b, c] = outs[b]

    with jax.named_scope("drain"):
        drain("f")
        proj_ref[...] = small_ref[:block, :earlier]
        tri_ref[...] = small_ref[ROWS:ROWS + block, :block]


def hand_over(new_in, proj_in, tri_in, new_out, proj_out, tri_out, sem):
    pairs = ((new_in, new_out), (proj_in, proj_out), (tri_in, tri_out))
    copies = [pltpu.make_async_copy(*pair, sem.at[at]) for at, pair in enumerate(pairs)]
    for copy in copies:
        copy.start()
    for copy in copies:
        copy.wait()


def body(sizes, coefficients, earlier, start, shifts):
    coefficients = jnp.transpose(coefficients, (0, 1, 2, 4, 3, 5))
    earlier = jnp.transpose(earlier, (0, 1, 3, 2, 4))
    start = jnp.transpose(start, (0, 2, 1, 3))
    depth, count = shifts.shape[0], earlier.shape[0]
    block = depth + 1
    kinds, comp, _, width, rows, lanes = coefficients.shape
    rounds = len(steps_of(depth))
    late = block - steps_of(depth)[-1]
    lines = late // 2 + late % 2
    single, joint = stages_of(sizes), joint_stages_of(sizes)
    most = max(members(stage) for stage in single)
    joined = max(members(stage) for stage in joint)
    levels = max(1, levels_of([n for _, n in sizes]))
    f32, b16 = jnp.float32, jnp.bfloat16
    anywhere = pl.BlockSpec(memory_space=pl.ANY)
    vmem = pl.BlockSpec(memory_space=pltpu.VMEM)
    sems = pltpu.SemaphoreType.DMA
    found = pl.pallas_call(
        functools.partial(kernel, sizes),
        out_shape=(
            pltpu.VMEM((block, comp, width, rows, lanes), f32),
            pltpu.VMEM((block, count), f32),
            pltpu.VMEM((block, block), f32),
        ),
        in_specs=[anywhere] * 4,
        out_specs=(vmem, vmem, vmem),
        scratch_shapes=[
            pltpu.VMEM(coefficients.shape, coefficients.dtype),
            pltpu.VMEM(coefficients.shape, f32),
            pltpu.VMEM((comp, comp, rows, lanes), f32),
            pltpu.VMEM((2, comp, comp, rows, lanes), b16),
            pltpu.VMEM((2, 4 * comp * comp, lanes), b16),
            pltpu.VMEM((2, 4 * comp * comp, lanes), b16),
            pltpu.VMEM((comp, comp, rows, lanes), f32),
            pltpu.VMEM((count + block, comp, width, rows, lanes), f32),
            pltpu.VMEM((3, comp, count * rows, width * lanes), b16),
            pltpu.VMEM((rounds, comp, width, rows, lanes), f32),
            pltpu.VMEM((comp, width, rows, lanes), f32),
            pltpu.VMEM((rounds, 2, 2, comp, rows, lanes), f32),
            pltpu.VMEM((rounds, 2, 2, 4 * comp, lanes), f32),
            pltpu.VMEM((rounds, 2, 2, 4 * comp, lanes), f32),
            pltpu.VMEM((rounds, 2, 2, 2 * rows, lanes), f32),
            pltpu.VMEM((rounds, 2, 2, 2 * rows, lanes), f32),
            pltpu.VMEM((2, comp, rows, lanes), f32),
            pltpu.VMEM((comp, rows, lanes), f32),
            pltpu.VMEM((2, comp, rows, lanes), f32),
            pltpu.VMEM((comp, rows, lanes), f32),
            pltpu.VMEM((count * rows, count * rows), f32),
            pltpu.VMEM((count * rows, count * rows), f32),
            pltpu.VMEM((lines, lanes, lanes), f32),
            pltpu.VMEM((lanes, lanes), f32),
            pltpu.VMEM((2 * rows, lanes), f32),
            pltpu.VMEM((2, block, rows, lanes), f32),
            pltpu.VMEM((len(single) + 1, rows + 1, lanes), f32),
            pltpu.VMEM((len(single), most, rows + 1, lanes), f32),
            pltpu.VMEM((len(joint) + 1, max(1, lines - 1), 1, lanes), f32),
            pltpu.VMEM((len(joint), joined, max(1, lines - 1), 1, lanes), f32),
            pltpu.VMEM((len(joint) + 1, 1, lanes), f32),
            pltpu.VMEM((len(joint), joined, 1, lanes), f32),
            sems((6,)),
            sems((2, 2, 2)),
            sems((2, 2, 2, 2)),
            sems((2, 2)),
            sems((2, 2, 2)),
            sems((2, 2)),
            sems((2, 2)),
            sems((len(single),)),
            sems((len(single),)),
            sems((len(joint),)),
            sems((len(joint),)),
            sems((len(joint),)),
            sems((len(joint),)),
            pltpu.SemaphoreType.REGULAR((levels,)),
            pltpu.SMEM(shifts.shape, f32),
        ],
        compiler_params=pltpu.CompilerParams(collective_id=0, has_side_effects=True),
        name="powers",
    )(coefficients, earlier, start, shifts)
    found = [pltpu.with_memory_space_constraint(value, pltpu.VMEM) for value in found]
    new, proj, tri = pl.pallas_call(
        hand_over,
        out_shape=[jax.ShapeDtypeStruct(value.shape, f32) for value in found],
        in_specs=[vmem] * 3,
        out_specs=[anywhere] * 3,
        scratch_shapes=[sems((3,))],
        name="hand_over",
    )(*found)
    return jnp.transpose(new, (0, 1, 3, 2, 4)), proj.T, tri


def solution(mesh):
    sizes = (("slab", mesh.shape["slab"]), ("sub", mesh.shape["sub"]))
    placed = (
        P(None, None, None, "slab", "sub", None),
        P(None, None, "slab", "sub", None),
        P(None, "slab", "sub", None),
        P(),
    )
    return jax.shard_map(
        functools.partial(body, sizes),
        mesh=mesh,
        in_specs=placed,
        out_specs=(P(None, None, "slab", "sub", None), P(), P()),
        check_vma=False,
    )
```

```python
import functools

import jax
import jax.numpy as jnp
from jax import lax
from jax.experimental import pallas as pl
from jax.experimental.pallas import tpu as pltpu
from jax.sharding import PartitionSpec as P

MESH = pl.DeviceIdType.MESH
LANES = 128
ROWS = 8
REACH = (2, 1)


def dot(a, b, nt=False):
    return lax.dot_general(
        a, b, (((1,), (1 if nt else 0,)), ((), ())),
        precision=lax.Precision.HIGHEST, preferred_element_type=jnp.float32,
    )


def iota(shape, dim):
    return lax.broadcasted_iota(jnp.int32, shape, dim)


def onehot(shape, test):
    return jnp.where(test(iota(shape, 0), iota(shape, 1)), 1.0, 0.0).astype(jnp.float32)


def diagonal(value):
    r, q = iota(value.shape, 0), iota(value.shape, 1)
    return jnp.where((r & 7) == (q & 7), value, 0.0)


def split(value):
    first = value.astype(jnp.bfloat16)
    left = value - first.astype(jnp.float32)
    second = left.astype(jnp.bfloat16)
    third = (left - second.astype(jnp.float32)).astype(jnp.bfloat16)
    return [first, second, third]


def dot_pieces(a, b, nt=False):
    found = None
    rows = a[0].shape[0]
    for at in (2, 1, 0):
        left = jnp.concatenate(a[: 3 - at], axis=0)
        part = lax.dot_general(
            left, b[at], (((1,), (1 if nt else 0,)), ((), ())),
            preferred_element_type=jnp.float32,
        )
        for i in reversed(range(3 - at)):
            piece = part[i * rows:(i + 1) * rows]
            found = piece if found is None else found + piece
    return found


def side_by_side(value):
    count, width = value.shape[0], value.shape[1]
    return jnp.concatenate(
        [value[:, x].reshape(count * ROWS, LANES) for x in range(width)], axis=1
    )


def factors(count):
    found = []
    while count > 1:
        fits = [f for f in range(2, min(count, 8) + 1) if count % f == 0]
        found.append(max(fits) if fits else count)
        count //= found[-1]
    return found


def stages_of(sizes):
    found = []
    for at, (_, count) in enumerate(sizes):
        stride = 1
        for size in factors(count):
            found.append(((stride, size), (1, 1)) if at == 0 else ((1, 1), (stride, size)))
            stride *= size
    return found


def joint_stages_of(sizes):
    slabs, subs = stages_of(sizes[:1]), [s[1] for s in stages_of((("", 1), sizes[1]))]
    first = slabs[0][0] if slabs else (1, 1)
    found = [(first, subs[0] if subs else (1, 1))]
    found += [(s[0], (1, 1)) for s in slabs[1:]] + [((1, 1), s) for s in subs[1:]]
    return found


def levels_of(extent):
    levels = 0
    while any(reach << levels < n - 1 for reach, n in zip(REACH, extent)):
        levels += 1
    return levels


def members(stage):
    return stage[0][1] * stage[1][1]


def offsets_of(stage):
    return [(a, b) for a in range(stage[0][1]) for b in range(stage[1][1]) if a or b]


def steps_of(depth):
    return ([1] if depth % 2 else []) + [2] * (depth // 2)


def lane_sums(value):
    return jnp.sum(value, axis=1, keepdims=True)


def sublane_sums(value):
    for shift in (4, 2, 1):
        value = value + pltpu.roll(value, shift, 0)
    return value


def inverse_root(value):
    scale = lax.rsqrt(value)
    return scale * (1.5 - 0.5 * value * scale * scale)


def kernel(
    sizes, coef_hbm, early_hbm, start_hbm, shifts_hbm, new_ref, proj_ref, tri_ref,
    coef_in, coef, edge_coef, gx_in, gz_send, gz_in, gz, allv, pieces, part, acc_ref,
    halo_x, halo_z, send_z, send_c, halo_c, pre_x, pre_z, ghost_x, ghost_z,
    edge_ref, ee, ee_cross, sums_ref, late_ref, small_ref, change_ref,
    mine_ee, gathered_ee, mine_b, gathered_b, mine_f, gathered_f,
    in_sem, face_send, face_recv, corner_send, corner_recv, g_recv,
    ee_send, ee_recv, b_send, b_recv, f_send, f_recv, ready, shifts_ref,
):
    depth = shifts_ref.shape[0]
    earlier, comp, width = early_hbm.shape[:3]
    block = depth + 1
    count = comp * width * ROWS * LANES * sizes[0][1] * sizes[1][1]
    half = LANES // 2
    rounds = steps_of(depth)
    paired = [r for r, size in enumerate(rounds) if size == 2]
    single = stages_of(sizes)[::-1]
    joint = joint_stages_of(sizes)
    place = [lax.axis_index(axis) for axis, _ in sizes]
    extent = [n for _, n in sizes]
    names = [axis for axis, _ in sizes]
    late = block - rounds[-1]
    lines = late // 2 + late % 2

    copy_start = pltpu.make_async_copy(start_hbm, allv.at[earlier], in_sem.at[0])
    def coef_part(low, high, sem):
        part = pl.ds(low, high - low)
        return pltpu.make_async_copy(coef_hbm.at[part], coef_in.at[part], in_sem.at[sem])

    kinds = coef_hbm.shape[0]
    copy_height, copy_rest = coef_part(1, 3, 1), [coef_part(3, kinds, 4), coef_part(0, 1, 5)]
    copy_early = pltpu.make_async_copy(early_hbm, allv.at[pl.ds(0, earlier)], in_sem.at[2])
    copy_shifts = pltpu.make_async_copy(shifts_hbm, shifts_ref, in_sem.at[3])
    copy_start.start()
    copy_shifts.start()
    copy_height.start()
    for copy in copy_rest:
        copy.start()

    def there(kind, side, sending):
        upward = (side == 0) == sending
        return place[kind] < extent[kind] - 1 if upward else place[kind] > 0

    def at_peer(dz, dx):
        return {names[0]: place[0] + dz, names[1]: place[1] + dx}

    def toward(side):
        return 1 if side == 0 else -1

    def peer(stage, offset):
        mine_at, peer_at, target = [], [], {}
        for axis in (0, 1):
            stride, size = stage[axis]
            digit = lax.rem(place[axis] // stride, size)
            other = lax.rem(digit + offset[axis], size)
            mine_at.append(digit)
            peer_at.append(other)
            target[names[axis]] = place[axis] + (other - digit) * stride
        flat = stage[1][1]
        return mine_at[0] * flat + mine_at[1], peer_at[0] * flat + peer_at[1], target

    levels = levels_of(extent)

    def around(reach, unit, act):
        for dz in range(-reach[0], reach[0] + 1):
            for dx in range(-reach[1], reach[1] + 1):
                far = (unit[0] * dz, unit[1] * dx)
                if far != (0, 0):
                    a, b = place[0] + far[0], place[1] + far[1]

                    @pl.when((a >= 0) & (a < extent[0]) & (b >= 0) & (b < extent[1]))
                    def _():
                        act(at_peer(*far))

    def signal(sem):
        return lambda where: pl.semaphore_signal(
            sem, inc=1, device_id=where, device_id_type=MESH
        )

    def wait_around(sem, reach, unit):
        total = 1
        for axis in (0, 1):
            seen = 1
            for d in range(1, reach[axis] + 1):
                far = d * unit[axis]
                seen = seen + jnp.where(place[axis] >= far, 1, 0)
                seen = seen + jnp.where(place[axis] + far < extent[axis], 1, 0)
            total = total * seen
        pl.semaphore_wait(sem, total - 1)

    def greet(level):
        if 0 < level <= levels:
            unit = tuple(x << (level - 1) for x in REACH)
            wait_around(ready.at[level - 1], (1, 1), unit)
        if level < levels:
            unit = tuple(x << level for x in REACH)
            around((1, 1), unit, signal(ready.at[level]))

    barrier = pltpu.get_barrier_semaphore()
    around(REACH, (1, 1), signal(barrier))

    for kind in (0, 1):
        for side in (0, 1):
            @pl.when(jnp.logical_not(there(kind, side, False)))
            def _():
                halo, coupling = (halo_z, gz_in) if kind == 0 else (halo_x, gx_in)
                for r in range(len(rounds)):
                    for what in (0, 1):
                        halo[r, what, side] = jnp.zeros_like(halo[r, what, side])
                coupling[side] = jnp.zeros_like(coupling[side])
    for sz in (0, 1):
        for sx in (0, 1):
            @pl.when(jnp.logical_not(there(0, sz, False) & there(1, sx, False)))
            def _():
                for r in range(len(rounds)):
                    halo_c[r, sz, sx] = jnp.zeros_like(halo_c[r, sz, sx])

    edge_ref[...] = jnp.zeros_like(edge_ref)
    edge_coef[...] = jnp.zeros_like(edge_coef)
    ee[...] = jnp.zeros_like(ee)
    ee_cross[...] = jnp.zeros_like(ee_cross)
    sums_ref[...] = jnp.zeros_like(sums_ref)
    late_ref[...] = jnp.zeros_like(late_ref)

    def face_copy(r, step, what, kind, side):
        if kind == 0:
            src, dst = send_z.at[r, what, side], halo_z.at[r, what, side]
        else:
            x = width - 1 if side == 0 else 0
            src = allv.at[earlier + step, :, x] if what == 0 else part.at[r, :, x]
            dst = halo_x.at[r, what, side]
        dz, dx = (toward(side), 0) if kind == 0 else (0, toward(side))
        return pltpu.make_async_remote_copy(
            src_ref=src, dst_ref=dst,
            send_sem=face_send.at[what, kind], recv_sem=face_recv.at[r % 2, what, kind],
            device_id=at_peer(dz, dx), device_id_type=MESH,
        )

    def corner_copy(r, sz, sx):
        return pltpu.make_async_remote_copy(
            src_ref=send_c.at[r, sz, sx], dst_ref=halo_c.at[r, sz, sx],
            send_sem=corner_send.at[0], recv_sem=corner_recv.at[r % 2],
            device_id=at_peer(toward(sz), toward(sx)), device_id_type=MESH,
        )

    def g_copy(kind, side):
        if kind == 0:
            src, dst = gz_send.at[side], gz_in.at[side]
        else:
            src = coef_in.at[4, :, :, width - 1] if side == 0 else coef_in.at[3, :, :, 0]
            dst = gx_in.at[side]
        dz, dx = (toward(side), 0) if kind == 0 else (0, toward(side))
        return pltpu.make_async_remote_copy(
            src_ref=src, dst_ref=dst, send_sem=face_send.at[1, kind],
            recv_sem=g_recv.at[kind], device_id=at_peer(dz, dx), device_id_type=MESH,
        )

    def each_face(sending, kinds, act):
        for kind in kinds:
            for side in (0, 1):
                @pl.when(there(kind, side, sending))
                def _():
                    act(kind, side)

    def each_corner(sending, act):
        for sz in (0, 1):
            for sx in (0, 1):
                @pl.when(there(0, sz, sending) & there(1, sx, sending))
                def _():
                    act(sz, sx)

    def amount(ref, send_sem, recv_sem, sending):
        copy = pltpu.make_async_remote_copy(
            src_ref=ref, dst_ref=ref, send_sem=send_sem, recv_sem=recv_sem,
            device_id=at_peer(0, 0), device_id_type=MESH,
        )
        return copy.wait_send if sending else copy.wait_recv

    def both(kind, sending):
        return there(kind, 0, sending) & there(kind, 1, sending)

    def single_side(kind, sending):
        return there(kind, 0, sending) ^ there(kind, 1, sending)

    def wait_faces(r, what, kinds, sending):
        for kind in kinds:
            halo = (halo_z, halo_x)[kind]
            sems = (face_send.at[what, kind], face_recv.at[r % 2, what, kind], sending)
            pl.when(both(kind, sending))(lambda: amount(halo.at[r, what], *sems)())
            pl.when(single_side(kind, sending))(lambda: amount(halo.at[r, what, 0], *sems)())

    def wait_corners(r, sending):
        sems = (corner_send.at[0], corner_recv.at[r % 2], sending)
        two = [both(kind, sending) for kind in (0, 1)]
        one = [single_side(kind, sending) for kind in (0, 1)]
        pl.when(two[0] & two[1])(lambda: amount(halo_c.at[r], *sems)())
        pl.when((two[0] & one[1]) | (one[0] & two[1]))(lambda: amount(halo_c.at[r, 0], *sems)())
        pl.when(one[0] & one[1])(lambda: amount(halo_c.at[r, 0, 0], *sems)())

    def wait_couplings(sending):
        for kind in (0, 1):
            held = (gz_in, gx_in)[kind]
            sems = (face_send.at[1, kind], g_recv.at[kind], sending)
            pl.when(both(kind, sending))(lambda: amount(held, *sems)())
            pl.when(single_side(kind, sending))(lambda: amount(held.at[0], *sems)())

    def pack(r, what, source):
        for e in range(comp):
            for x in range(width):
                row = width * e + x
                tile = source(e, x)
                send_z[r, what, 0, row:row + 1, :] = tile[ROWS - 1:ROWS, :]
                send_z[r, what, 1, row:row + 1, :] = tile[0:1, :]

    def send_faces(r, step):
        pack(r, 0, lambda e, x: allv.at[earlier + step, e, x])
        each_face(True, (0, 1), lambda kind, side: face_copy(r, step, 0, kind, side).start())

    row2 = iota((ROWS, LANES), 0)
    row3 = iota((width, ROWS, LANES), 1)
    lane3 = iota((width, ROWS, LANES), 2)
    zero_tile = jnp.zeros((1, ROWS, LANES), jnp.float32)
    low_rows = row2 < 4

    def split_pair(below, above, odd):
        if odd:
            return jnp.where(low_rows, pltpu.roll(below, 4, 0), above)
        return jnp.where(low_rows, below, pltpu.roll(above, 4, 0))

    def spread_edges(below, above):
        for e in range(comp):
            for x in range(width):
                at = width * e + x
                edge_ref[e, x:x + 1, :] = below[at:at + 1, :]
                edge_ref[e, 4 + x:5 + x, :] = above[at:at + 1, :]

    def apply_local(step):
        acc = 0.0
        for e in range(comp):
            v = allv[earlier + step, e]
            near = [
                v,
                jnp.where(row3 > 0, pltpu.roll(v, 1, 1), 0.0),
                jnp.where(row3 < ROWS - 1, pltpu.roll(v, ROWS - 1, 1), 0.0),
                jnp.concatenate([zero_tile, v[:-1]], axis=0),
                jnp.concatenate([v[1:], zero_tile], axis=0),
                jnp.where(lane3 > 0, pltpu.roll(v, 1, 2), 0.0),
                jnp.where(lane3 < LANES - 1, pltpu.roll(v, LANES - 1, 2), 0.0),
            ]
            for d in range(len(near)):
                acc = acc + coef[d, :, e] * near[d][None]
        return acc

    def add_x(source, x_of):
        found = []
        for side, d, x in ((0, 3, 0), (1, 4, width - 1)):
            value = source(x)
            for e in range(comp):
                value = value + coef[d, :, e, x] * x_of(side, e)[None]
            found.append(value)
        return found

    def add_z(z_of):
        edge = jnp.zeros((comp, ROWS, LANES), jnp.float32)
        for e in range(comp):
            edge = edge + edge_coef[:, e] * z_of(e)[None]
        return edge

    def store_step(step, source, sides, edge):
        for c in range(comp):
            for x in range(width):
                value = sides[0][c] if x == 0 else sides[1][c] if x == width - 1 else source(x)[c]
                value = value + jnp.where(
                    row2 == 0, edge[c, x:x + 1, :],
                    jnp.where(row2 == ROWS - 1, edge[c, 4 + x:5 + x, :], 0.0),
                )
                allv[earlier + step, c, x] = value

    def take_faces(r, step, source):
        wait_faces(r, 0, (1,), False)
        sides = add_x(source, lambda side, e: halo_x[r, 0, side, e])
        wait_faces(r, 0, (0,), False)
        spread_edges(halo_z.at[r, 0, 0], halo_z.at[r, 0, 1])
        edge = add_z(lambda e: edge_ref[e])
        store_step(step + 1, source, sides, edge)

    def cross_products(k, ref, base):
        total, group = earlier + k + 1, 6
        w = allv[earlier + k]
        for low in range(0, total, group):
            high = min(low + group, total)
            sums = jnp.sum(w[None] * allv[low:high], axis=(1, 2))
            ref[base + low:base + high, :] = jnp.sum(sums, axis=1)

    def as_line(value):
        return jnp.sum(value.T, axis=0, keepdims=True)

    def times(a, b):
        return lax.dot_general(
            a, b, (((1,), (1,)), ((), ())), preferred_element_type=jnp.float32
        )

    def self_products(c):
        parts = split(side_by_side(allv[pl.ds(0, earlier), c]))
        for at, piece in enumerate(parts):
            pieces[at, c] = piece
        one = times(parts[0], parts[0])
        two = times(jnp.concatenate(parts[:2], axis=0), parts[1])
        three = times(parts[0], parts[2])
        span = earlier * ROWS
        ee[...] += one + two[span:]
        ee_cross[...] += two[:span] + three

    def gather_self(value):
        span = earlier * ROWS
        rows = jnp.sum(diagonal(value).reshape(earlier, ROWS, span), axis=1)
        own = onehot((span, LANES), lambda r, q: (r >> 3) == q).astype(jnp.bfloat16)
        found = None
        for piece in split(rows)[::-1]:
            some = lax.dot_general(
                piece, own, (((1,), (0,)), ((), ())), preferred_element_type=jnp.float32
            )
            found = some if found is None else found + some
        return jnp.concatenate(
            [found, jnp.zeros((LANES - earlier, LANES), jnp.float32)], axis=0
        )

    def self_finish():
        cross = gather_self(ee_cross[...])
        whole = gather_self(ee[...])[:32] + (cross + cross.T)[:32]
        packed = whole[:ROWS]
        for g in range(1, 4):
            packed = packed + pltpu.roll(whole[ROWS * g:ROWS * (g + 1)], 32 * g, 1)
        mine_ee[0, :ROWS] = packed
        mine_ee[0, ROWS:] = as_line(sums_ref[0])

    exchanges = {
        "ee": (single, mine_ee, gathered_ee, ee_send, ee_recv),
        "b": (joint, mine_b, gathered_b, b_send, b_recv),
        "f": (joint, mine_f, gathered_f, f_send, f_recv),
    }

    def begin(name, at):
        stages, own, slots, send_sem, recv_sem = exchanges[name]
        for offset in offsets_of(stages[at]):
            here, _, target = peer(stages[at], offset)
            pltpu.make_async_remote_copy(
                src_ref=own.at[at], dst_ref=slots.at[at, here],
                send_sem=send_sem.at[at], recv_sem=recv_sem.at[at],
                device_id=target, device_id_type=MESH,
            ).start()

    def all_of(name, at):
        stages, own, slots, send_sem, recv_sem = exchanges[name]
        others = slots.at[at, pl.ds(0, members(stages[at]) - 1)]
        _, _, target = peer(stages[at], offsets_of(stages[at])[0])
        return pltpu.make_async_remote_copy(
            src_ref=others, dst_ref=others, send_sem=send_sem.at[at], recv_sem=recv_sem.at[at],
            device_id=target, device_id_type=MESH,
        )

    def finish(name, at):
        stages, own, slots, _, _ = exchanges[name]
        here, _, _ = peer(stages[at], (0, 0))
        slots[at, here] = own[at]
        all_of(name, at).wait_recv()
        whole = slots[at, 0]
        for other in range(1, members(stages[at])):
            whole = whole + slots[at, other]
        own[at + 1] = whole

    def drain(name):
        for at in range(len(exchanges[name][0])):
            all_of(name, at).wait_send()

    def whole_exchange(name, first):
        stages = exchanges[name][0]
        for at in range(len(stages)):
            if at or not first:
                begin(name, at)
            finish(name, at)
        return exchanges[name][1][len(stages)] * (1.0 / count)

    def load_height():
        @pl.loop(0, comp)
        def _(c):
            for d in (1, 2):
                coef[d, c] = coef_in[d, c].astype(jnp.float32)
            for e in range(comp):
                for x in range(width):
                    edge_coef[c, e, x:x + 1, :] = coef[1, c, e, x, 0:1, :]
                    edge_coef[c, e, 4 + x:5 + x, :] = coef[2, c, e, x, ROWS - 1:ROWS, :]

        flat = comp * comp // 2
        for low in range(0, flat, 2):
            for side in (0, 1):
                both = []
                for at in (low, low + 1):
                    c, e = 2 * at // comp, 2 * at % comp
                    one, two = edge_coef[c, e], edge_coef[c, e + 1]
                    if side == 0:
                        both.append(jnp.where(low_rows, pltpu.roll(one, 4, 0), two))
                    else:
                        both.append(jnp.where(low_rows, one, pltpu.roll(two, 4, 0)))
                gz_send[side, ROWS * low:ROWS * (low + 2), :] = jnp.concatenate(
                    both, axis=0
                ).astype(jnp.bfloat16)

    def load_rest():
        @pl.loop(0, comp)
        def _(c):
            for d in (0, *range(3, coef.shape[0])):
                coef[d, c] = coef_in[d, c].astype(jnp.float32)

    def take_couplings():
        wait_couplings(False)
        for low in range(0, comp * comp // 2, 2):
            below = gz_in[0, ROWS * low:ROWS * (low + 2), :].astype(jnp.float32)
            above = gz_in[1, ROWS * low:ROWS * (low + 2), :].astype(jnp.float32)
            for at in (0, 1):
                c, e = 2 * (low + at) // comp, 2 * (low + at) % comp
                b, a = below[ROWS * at:ROWS * (at + 1)], above[ROWS * at:ROWS * (at + 1)]
                gz[c, e] = split_pair(b, a, 0)
                gz[c, e + 1] = split_pair(b, a, 1)

    def complete_neighbours(r, step):
        for side, x in ((0, 0), (1, width - 1)):
            for c in range(comp):
                value = jnp.zeros((ROWS, LANES), jnp.float32)
                for e in range(comp):
                    value = value + gx_in[side, c, e].astype(jnp.float32) * allv[earlier + step, e, x]
                pre_x[side, c] = value
        total = jnp.zeros((comp, ROWS, LANES), jnp.float32)
        spread_edges(send_z.at[r, 0, 1], send_z.at[r, 0, 0])
        for e in range(comp):
            total = total + gz[:, e] * edge_ref[e][None]
        pre_z[...] = total
        for sz in (0, 1):
            for sx in (0, 1):
                z = ROWS - 1 if sz == 0 else 0
                x = (4 if sz == 0 else 0) + (width - 1 if sx == 0 else 0)
                for c in range(comp):
                    send_c[r, sz, sx, c:c + 1, :] = pre_x[1 - sx, c, z:z + 1, :]
                    send_c[r, sz, sx, comp + c:comp + c + 1, :] = pre_z[c, x:x + 1, :]
        each_corner(True, lambda sz, sx: corner_copy(r, sz, sx).start())

    def take_ghosts(r, step):
        wait_faces(r, 1, (1, 0), False)
        wait_corners(r, False)
        spread_edges(halo_z.at[r, 1, 0], halo_z.at[r, 1, 1])
        for c in range(comp):
            value = edge_ref[c] + pre_z[c]
            for sz in (0, 1):
                for sx in (0, 1):
                    row = (0 if sz == 0 else 4) + (0 if sx == 0 else width - 1)
                    value = value + jnp.where(row2 == row, halo_c[r, sz, sx, c:c + 1, :], 0.0)
            ghost_z[c] = value
            for side in (0, 1):
                value = halo_x[r, 1, side, c] + pre_x[side, c]
                for sz in (0, 1):
                    row = 0 if sz == 0 else ROWS - 1
                    value = value + jnp.where(
                        row2 == row, halo_c[r, sz, side, comp + c:comp + c + 1, :], 0.0
                    )
                ghost_x[side, c] = value

    with jax.named_scope("start"):
        copy_start.wait()
        copy_early.start()
        wait_around(barrier, REACH, (1, 1))
        greet(0)

    step = 0
    comps = list(range(comp))
    before = max(1, len(rounds) - 1)
    share = [2 * comp // (before + 1)] + [comp // (before + 1)] * (before - 1)
    share[-1] += comp - sum(share)
    share += [0] * (len(rounds) - len(share))
    greeted, ee_at, self_at, done = 1, None, 0, 0

    def self_some(low, high):
        @pl.loop(low, high)
        def _(c):
            self_products(c)

    for r, size in enumerate(rounds):
        with jax.named_scope(f"send{r}"):
            if r:
                wait_faces(r - 1, 0, (0, 1), True)
            send_faces(r, step)
        if r == 0:
            with jax.named_scope("load"):
                copy_height.wait()
                load_height()
                each_face(True, (0,) if paired else (), lambda kind, side: g_copy(kind, side).start())
                for copy in copy_rest:
                    copy.wait()
                each_face(True, (1,) if paired else (), lambda kind, side: g_copy(kind, side).start())
                load_rest()
        with jax.named_scope(f"local{r}"):
            part[r] = apply_local(step)
        with jax.named_scope(f"part{r}"):
            if size == 2:
                pack(r, 1, lambda e, x: part.at[r, e, x])
                if r > paired[0]:
                    wait_faces(r - 1, 1, (0, 1), True)
                else:
                    wait_couplings(True)
                each_face(True, (0, 1), lambda kind, side: face_copy(r, step, 1, kind, side).start())
        with jax.named_scope(f"neigh{r}"):
            if size == 2 and r == paired[0]:
                take_couplings()
            if size == 2:
                if r > paired[0]:
                    wait_corners(r - 1, True)
                complete_neighbours(r, step)
        with jax.named_scope(f"cross{r}"):
            if len(rounds) == 1:
                copy_early.wait()
            if r or len(rounds) == 1:
                for k in range(done, min(step + 1, late)):
                    cross_products(k, sums_ref.at[k // 2], (k % 2) * half)
                    done = k + 1
        with jax.named_scope(f"self{r}"):
            if share[r]:
                middle = self_at + share[r] // 2
                if r == 0:
                    if len(rounds) > 1:
                        copy_early.wait()
                    self_some(self_at, middle)
                    greet(greeted)
                    greeted += 1
                    self_some(middle, self_at + share[r])
                else:
                    if greeted <= levels:
                        greet(greeted)
                        greeted += 1
                    self_some(self_at, self_at + share[r])
                self_at += share[r]
        with jax.named_scope(f"ee{r}"):
            if done == late and r == len(rounds) - 1:
                for q in range(1, lines):
                    mine_b[0, q - 1] = as_line(sums_ref[q])
                begin("b", 0)
            if share[r] and self_at == comp:
                self_finish()
                while greeted <= levels:
                    greet(greeted)
                    greeted += 1
                begin("ee", 0)
                ee_at = 0
            elif ee_at == 0 and len(single) > 1:
                finish("ee", 0)
                begin("ee", 1)
                ee_at = 1
        with jax.named_scope(f"faces{r}"):
            take_faces(r, step, lambda x, r=r: part[r, :, x])
        if size == 2:
            with jax.named_scope(f"late{r}"):
                if r == len(rounds) - 1:
                    cross_products(step + 1, late_ref, 0)
            with jax.named_scope(f"second{r}"):
                acc_ref[...] = apply_local(step + 1)
            with jax.named_scope(f"ghost{r}"):
                take_ghosts(r, step)
            with jax.named_scope(f"store{r}"):
                sides = add_x(lambda x: acc_ref[:, x], lambda side, e: ghost_x[side, e])
                edge = add_z(lambda e: ghost_z[e])
                store_step(step + 2, lambda x: acc_ref[:, x], sides, edge)
        step += size

    with jax.named_scope("last"):
        cross_products(depth, late_ref, half)
        mine_f[0] = as_line(late_ref[...])
        begin("f", 0)

    with jax.named_scope("eewait"):
        for at in range(ee_at, len(single)):
            if at > ee_at:
                begin("ee", at)
            finish("ee", at)
        packed = mine_ee[len(single), :ROWS] * (1.0 / count)
        ahead = mine_ee[len(single), ROWS:] * (1.0 / count)
    row, lane = iota((ROWS, LANES), 0), iota((ROWS, LANES), 1)
    with jax.named_scope("change"):
        copy_shifts.wait()
        unit, nothing = jnp.ones((ROWS, LANES), jnp.float32), jnp.zeros((ROWS, LANES), jnp.float32)
        change = [[unit]]
        for k in range(depth):
            last, scale = change[-1], 1.0 - shifts_ref[k]
            change.append(
                [
                    (last[m - 1] if m else nothing) + (scale * last[m] if m <= k else nothing)
                    for m in range(k + 2)
                ]
            )
        for m in range(block):
            down, along = nothing, nothing
            for k in range(m, block):
                down = jnp.where(row == k, change[k][m], down)
                along = jnp.where(lane == k, change[k][m], along)
            change_ref[0, m] = down
            change_ref[1, m] = along
    with jax.named_scope("bwait"):
        early = whole_exchange("b", True)

    with jax.named_scope("algebra"):
        found = jnp.concatenate(
            [
                pltpu.roll(ahead if k < 2 else early[k // 2 - 1], (k % 2) * half, 1)
                for k in range(late)
            ] + [jnp.zeros((ROWS - late, LANES), jnp.float32)], axis=0
        )
        proj_t = jnp.where(lane < earlier, found, 0.0)
        known = jnp.where(lane < earlier + row, found, 0.0)
        pick = onehot((ROWS, LANES), lambda r, q: q == r + earlier)
        gram = jnp.where(lane <= earlier + row, found, 0.0)
        gram = pltpu.roll(gram, LANES - earlier, 1)[:, :ROWS]
        square = jnp.concatenate(
            [packed] + [pltpu.roll(packed, LANES - 32 * g, 1) for g in range(1, 4)], axis=0
        )
        sr, sl = iota(square.shape, 0), iota(square.shape, 1)
        inside = (sl < earlier) & (sr < earlier)
        square = jnp.where(inside, square - jnp.where(sr == sl, 2.0, 0.0), 0.0)
        moved = dot(proj_t[:, :32], square) + pick
        gram = gram + dot(moved, known, nt=True)

        upper = gram
        inverse = onehot((ROWS, ROWS), lambda r, q: (r == q) & (r < late))
        r8 = iota((ROWS, ROWS), 0)
        q8 = iota((ROWS, ROWS), 1)
        for p in range(late):
            pivot = upper[p:p + 1, p:p + 1]
            scale = inverse_root(pivot)
            column = upper[:, p:p + 1] * scale
            row_u, row_i = upper[p:p + 1, :] * scale, inverse[p:p + 1, :] * scale
            upper = jnp.where(r8 == p, row_u, jnp.where(r8 > p, upper - column * row_u, upper))
            inverse = jnp.where(r8 == p, row_i, jnp.where(r8 > p, inverse - column * row_i, inverse))
        onto = dot(inverse, moved)

        mix = dot(inverse, pick - proj_t)
        tall = jnp.concatenate(
            [jnp.broadcast_to(mix[k:k + 1], (ROWS, LANES)) for k in range(late)], axis=0
        )
        span = earlier * ROWS
        grow = onehot((LANES, span), lambda r, q: (q >> 3) == r).astype(jnp.bfloat16)
        mix = [
            diagonal(
                lax.dot_general(
                    piece, grow, (((1,), (0,)), ((), ())), preferred_element_type=jnp.float32
                )
            ).astype(jnp.bfloat16)
            for piece in split(tall)
        ]
        weights = [
            [
                jnp.broadcast_to(
                    tall[k * ROWS:(k + 1) * ROWS, earlier + i:earlier + i + 1], (ROWS, LANES)
                )
                for i in range(k + 1)
            ]
            for k in range(late)
        ]
    with jax.named_scope("out"):
        for c in range(comp):
            out = dot_pieces(mix, [pieces[at, c] for at in range(3)])
            for x in range(width):
                for k in range(late):
                    value = out[k * ROWS:(k + 1) * ROWS, LANES * x:LANES * (x + 1)]
                    for i in range(k + 1):
                        value = value + weights[k][i] * allv[earlier + i, c, x]
                    new_ref[k, c, x] = value
        proj_early, tri_early = 0.0, 0.0
        for m in range(late):
            proj_early = proj_early + change_ref[0, m] * proj_t[m:m + 1]
            column = jnp.where(r8[:, :1] <= m, upper[:, m:m + 1], 0.0)
            tri_early = tri_early + change_ref[1, m] * column
        small_ref[0:ROWS, :] = proj_early
        small_ref[ROWS:2 * ROWS, :] = jnp.where(row < late, tri_early, 0.0)

    with jax.named_scope("sent"):
        wait_faces(len(rounds) - 1, 0, (0, 1), True)
        if paired:
            wait_faces(paired[-1], 1, (0, 1), True)
            wait_corners(paired[-1], True)
        drain("ee")
        drain("b")
    with jax.named_scope("fwait"):
        final = whole_exchange("f", True)
    with jax.named_scope("columns"):
        ys = [final, pltpu.roll(final, half, 1)][2 - (block - late):]
        spread = [jnp.broadcast_to(y, (ROWS, LANES)) for y in ys]
        tiles = -(-(earlier + block) // ROWS)
        columns = []
        for y in spread:
            col = [
                lane_sums(jnp.where(lane == row + ROWS * t, y, 0.0)) for t in range(tiles)
            ]
            img = [
                lane_sums(square[ROWS * t:ROWS * (t + 1)] * y) for t in range(square.shape[0] // ROWS)
            ]
            columns.append((col, img, lane_sums(onto * y)))
        wide = lambda value: jnp.broadcast_to(value, (ROWS, LANES))

        def inner(a, b):
            (col_a, _, r_a), (col_b, img_b, r_b) = columns[a], columns[b]
            total = -(r_a * r_b)
            for t in range(len(img_b)):
                total = total + jnp.where(row[:, :1] + ROWS * t < earlier, col_a[t] * img_b[t], 0.0)
            for t in range(tiles):
                total = total + jnp.where(row[:, :1] + ROWS * t == earlier + late + a, col_b[t], 0.0)
            return sublane_sums(wide(total))

        fresh = block - late
        scales, ratios, lines_out = [], {}, []
        for b in range(fresh):
            value = inner(b, b)
            for a in range(b):
                cross = inner(a, b)
                ratios[a, b] = cross * scales[a]
                value = value - ratios[a, b] * ratios[a, b]
            scales.append(inverse_root(value))
            ratios[b, b] = value * scales[b]
        triangle = small_ref[ROWS:2 * ROWS, :]
        proj_rows = small_ref[0:ROWS, :]
        for b in range(fresh):
            column = wide(columns[b][2])
            for a in range(b + 1):
                column = jnp.where(row == late + a, ratios[a, b], column)
            triangle = triangle + change_ref[1, late + b] * column
            proj_rows = proj_rows + change_ref[0, late + b] * spread[b]
        small_ref[ROWS:2 * ROWS, :] = triangle
        small_ref[0:ROWS, :] = proj_rows
        for b in range(fresh):
            for t in range(tiles):
                late_ref[b * half + ROWS * t:b * half + ROWS * (t + 1), :] = wide(columns[b][0][t])
            late_ref[b * half + ROWS * tiles:b * half + ROWS * (tiles + 1), :] = wide(columns[b][2])

    with jax.named_scope("tail"):
        for c in range(comp):
            totals = [allv[earlier + late + b, c] for b in range(fresh)]
            for j in range(earlier):
                v = allv[j, c]
                for b in range(fresh):
                    at = b * half + j
                    totals[b] = totals[b] - late_ref[at:at + 1, :] * v
            for i in range(late):
                v = new_ref[i, c]
                for b in range(fresh):
                    at = b * half + ROWS * tiles + i
                    totals[b] = totals[b] - late_ref[at:at + 1, :] * v
            outs = []
            for b in range(fresh):
                value = totals[b]
                for a in range(b):
                    value = value - ratios[a, b] * outs[a]
                outs.append(value * scales[b])
                new_ref[late + b, c] = outs[b]

    with jax.named_scope("drain"):
        drain("f")
        proj_ref[...] = small_ref[:block, :earlier]
        tri_ref[...] = small_ref[ROWS:ROWS + block, :block]


def hand_over(new_in, proj_in, tri_in, new_out, proj_out, tri_out, sem):
    pairs = ((new_in, new_out), (proj_in, proj_out), (tri_in, tri_out))
    copies = [pltpu.make_async_copy(*pair, sem.at[at]) for at, pair in enumerate(pairs)]
    for copy in copies:
        copy.start()
    for copy in copies:
        copy.wait()


def body(sizes, coefficients, earlier, start, shifts):
    coefficients = jnp.transpose(coefficients, (0, 1, 2, 4, 3, 5))
    earlier = jnp.transpose(earlier, (0, 1, 3, 2, 4))
    start = jnp.transpose(start, (0, 2, 1, 3))
    depth, count = shifts.shape[0], earlier.shape[0]
    block = depth + 1
    kinds, comp, _, width, rows, lanes = coefficients.shape
    rounds = len(steps_of(depth))
    late = block - steps_of(depth)[-1]
    lines = late // 2 + late % 2
    single, joint = stages_of(sizes), joint_stages_of(sizes)
    most = max(members(stage) for stage in single)
    joined = max(members(stage) for stage in joint)
    levels = max(1, levels_of([n for _, n in sizes]))
    f32, b16 = jnp.float32, jnp.bfloat16
    anywhere = pl.BlockSpec(memory_space=pl.ANY)
    vmem = pl.BlockSpec(memory_space=pltpu.VMEM)
    sems = pltpu.SemaphoreType.DMA
    found = pl.pallas_call(
        functools.partial(kernel, sizes),
        out_shape=(
            pltpu.VMEM((block, comp, width, rows, lanes), f32),
            pltpu.VMEM((block, count), f32),
            pltpu.VMEM((block, block), f32),
        ),
        in_specs=[anywhere] * 4,
        out_specs=(vmem, vmem, vmem),
        scratch_shapes=[
            pltpu.VMEM(coefficients.shape, coefficients.dtype),
            pltpu.VMEM(coefficients.shape, f32),
            pltpu.VMEM((comp, comp, rows, lanes), f32),
            pltpu.VMEM((2, comp, comp, rows, lanes), b16),
            pltpu.VMEM((2, 4 * comp * comp, lanes), b16),
            pltpu.VMEM((2, 4 * comp * comp, lanes), b16),
            pltpu.VMEM((comp, comp, rows, lanes), f32),
            pltpu.VMEM((count + block, comp, width, rows, lanes), f32),
            pltpu.VMEM((3, comp, count * rows, width * lanes), b16),
            pltpu.VMEM((rounds, comp, width, rows, lanes), f32),
            pltpu.VMEM((comp, width, rows, lanes), f32),
            pltpu.VMEM((rounds, 2, 2, comp, rows, lanes), f32),
            pltpu.VMEM((rounds, 2, 2, width * comp, lanes), f32),
            pltpu.VMEM((rounds, 2, 2, width * comp, lanes), f32),
            pltpu.VMEM((rounds, 2, 2, 2 * comp, lanes), f32),
            pltpu.VMEM((rounds, 2, 2, 2 * comp, lanes), f32),
            pltpu.VMEM((2, comp, rows, lanes), f32),
            pltpu.VMEM((comp, rows, lanes), f32),
            pltpu.VMEM((2, comp, rows, lanes), f32),
            pltpu.VMEM((comp, rows, lanes), f32),
            pltpu.VMEM((comp, rows, lanes), f32),
            pltpu.VMEM((count * rows, count * rows), f32),
            pltpu.VMEM((count * rows, count * rows), f32),
            pltpu.VMEM((lines, lanes, lanes), f32),
            pltpu.VMEM((lanes, lanes), f32),
            pltpu.VMEM((2 * rows, lanes), f32),
            pltpu.VMEM((2, block, rows, lanes), f32),
            pltpu.VMEM((len(single) + 1, rows + 1, lanes), f32),
            pltpu.VMEM((len(single), most, rows + 1, lanes), f32),
            pltpu.VMEM((len(joint) + 1, max(1, lines - 1), 1, lanes), f32),
            pltpu.VMEM((len(joint), joined, max(1, lines - 1), 1, lanes), f32),
            pltpu.VMEM((len(joint) + 1, 1, lanes), f32),
            pltpu.VMEM((len(joint), joined, 1, lanes), f32),
            sems((6,)),
            sems((2, 2)),
            sems((2, 2, 2)),
            sems((1,)),
            sems((2,)),
            sems((2,)),
            sems((len(single),)),
            sems((len(single),)),
            sems((len(joint),)),
            sems((len(joint),)),
            sems((len(joint),)),
            sems((len(joint),)),
            pltpu.SemaphoreType.REGULAR((levels,)),
            pltpu.SMEM(shifts.shape, f32),
        ],
        compiler_params=pltpu.CompilerParams(collective_id=0, has_side_effects=True),
        name="powers",
    )(coefficients, earlier, start, shifts)
    found = [pltpu.with_memory_space_constraint(value, pltpu.VMEM) for value in found]
    new, proj, tri = pl.pallas_call(
        hand_over,
        out_shape=[jax.ShapeDtypeStruct(value.shape, f32) for value in found],
        in_specs=[vmem] * 3,
        out_specs=[anywhere] * 3,
        scratch_shapes=[sems((3,))],
        name="hand_over",
    )(*found)
    return jnp.transpose(new, (0, 1, 3, 2, 4)), proj.T, tri


def solution(mesh):
    sizes = (("slab", mesh.shape["slab"]), ("sub", mesh.shape["sub"]))
    placed = (
        P(None, None, None, "slab", "sub", None),
        P(None, None, "slab", "sub", None),
        P(None, "slab", "sub", None),
        P(),
    )
    return jax.shard_map(
        functools.partial(body, sizes),
        mesh=mesh,
        in_specs=placed,
        out_specs=(P(None, None, "slab", "sub", None), P(), P()),
        check_vma=False,
    )
```

```python
import functools

import jax
import jax.numpy as jnp
from jax import lax
from jax.experimental import pallas as pl
from jax.experimental.pallas import tpu as pltpu
from jax.sharding import PartitionSpec as P

MESH = pl.DeviceIdType.MESH
LANES = 128
ROWS = 8
REACH = (2, 1)


def dot(a, b, nt=False):
    return lax.dot_general(
        a, b, (((1,), (1 if nt else 0,)), ((), ())),
        precision=lax.Precision.HIGHEST, preferred_element_type=jnp.float32,
    )


def iota(shape, dim):
    return lax.broadcasted_iota(jnp.int32, shape, dim)


def onehot(shape, test):
    return jnp.where(test(iota(shape, 0), iota(shape, 1)), 1.0, 0.0).astype(jnp.float32)


def diagonal(value):
    r, q = iota(value.shape, 0), iota(value.shape, 1)
    return jnp.where((r & 7) == (q & 7), value, 0.0)


def split(value):
    first = value.astype(jnp.bfloat16)
    left = value - first.astype(jnp.float32)
    second = left.astype(jnp.bfloat16)
    third = (left - second.astype(jnp.float32)).astype(jnp.bfloat16)
    return [first, second, third]


def dot_pieces(a, b, nt=False):
    found = None
    rows = a[0].shape[0]
    for at in (2, 1, 0):
        left = jnp.concatenate(a[: 3 - at], axis=0)
        part = lax.dot_general(
            left, b[at], (((1,), (1 if nt else 0,)), ((), ())),
            preferred_element_type=jnp.float32,
        )
        for i in reversed(range(3 - at)):
            piece = part[i * rows:(i + 1) * rows]
            found = piece if found is None else found + piece
    return found


def side_by_side(value):
    count, width = value.shape[0], value.shape[1]
    return jnp.concatenate(
        [value[:, x].reshape(count * ROWS, LANES) for x in range(width)], axis=1
    )


def factors(count):
    found = []
    while count > 1:
        fits = [f for f in range(2, min(count, 8) + 1) if count % f == 0]
        found.append(max(fits) if fits else count)
        count //= found[-1]
    return found


def stages_of(sizes):
    found = []
    for at, (_, count) in enumerate(sizes):
        stride = 1
        for size in factors(count):
            found.append(((stride, size), (1, 1)) if at == 0 else ((1, 1), (stride, size)))
            stride *= size
    return found


def joint_stages_of(sizes):
    slabs, subs = stages_of(sizes[:1]), [s[1] for s in stages_of((("", 1), sizes[1]))]
    first = slabs[0][0] if slabs else (1, 1)
    found = [(first, subs[0] if subs else (1, 1))]
    found += [(s[0], (1, 1)) for s in slabs[1:]] + [((1, 1), s) for s in subs[1:]]
    return found


def levels_of(extent):
    levels = 0
    while any(reach << levels < n - 1 for reach, n in zip(REACH, extent)):
        levels += 1
    return levels


def members(stage):
    return stage[0][1] * stage[1][1]


def offsets_of(stage):
    return [(a, b) for a in range(stage[0][1]) for b in range(stage[1][1]) if a or b]


def steps_of(depth):
    return ([1] if depth % 2 else []) + [2] * (depth // 2)


def lane_sums(value):
    return jnp.sum(value, axis=1, keepdims=True)


def sublane_sums(value):
    for shift in (4, 2, 1):
        value = value + pltpu.roll(value, shift, 0)
    return value


def inverse_root(value):
    scale = lax.rsqrt(value)
    return scale * (1.5 - 0.5 * value * scale * scale)


def kernel(
    sizes, coef_hbm, early_hbm, start_hbm, shifts_hbm, new_ref, proj_ref, tri_ref,
    coef_in, coef, edge_coef, gx_in, gz_send, gz_in, flat_ref, gz, allv, pieces, part, acc_ref,
    halo_x, halo_z, send_z, send_c, halo_c, pre_x, pre_z, ghost_x, ghost_z,
    edge_ref, ee, ee_cross, sums_ref, late_ref, small_ref, change_ref,
    mine_ee, gathered_ee, mine_b, gathered_b, mine_f, gathered_f,
    in_sem, face_send, face_recv, corner_send, corner_recv, g_recv,
    ee_send, ee_recv, b_send, b_recv, f_send, f_recv, ready, shifts_ref,
):
    depth = shifts_ref.shape[0]
    earlier, comp, width = early_hbm.shape[:3]
    block = depth + 1
    count = comp * width * ROWS * LANES * sizes[0][1] * sizes[1][1]
    half = LANES // 2
    rounds = steps_of(depth)
    paired = [r for r, size in enumerate(rounds) if size == 2]
    single = stages_of(sizes)[::-1]
    joint = joint_stages_of(sizes)
    place = [lax.axis_index(axis) for axis, _ in sizes]
    extent = [n for _, n in sizes]
    names = [axis for axis, _ in sizes]
    late = block - rounds[-1]
    lines = late // 2 + late % 2

    copy_start = pltpu.make_async_copy(start_hbm, allv.at[earlier], in_sem.at[0])
    def coef_part(low, high, sem):
        part = pl.ds(low, high - low)
        return pltpu.make_async_copy(coef_hbm.at[part], coef_in.at[part], in_sem.at[sem])

    kinds = coef_hbm.shape[0]
    copy_height, copy_rest = coef_part(1, 3, 1), [coef_part(3, kinds, 4), coef_part(0, 1, 5)]
    copy_early = pltpu.make_async_copy(early_hbm, allv.at[pl.ds(0, earlier)], in_sem.at[2])
    copy_shifts = pltpu.make_async_copy(shifts_hbm, shifts_ref, in_sem.at[3])
    copy_start.start()
    copy_shifts.start()
    copy_height.start()
    for copy in copy_rest:
        copy.start()

    def there(kind, side, sending):
        upward = (side == 0) == sending
        return place[kind] < extent[kind] - 1 if upward else place[kind] > 0

    def at_peer(dz, dx):
        return {names[0]: place[0] + dz, names[1]: place[1] + dx}

    def toward(side):
        return 1 if side == 0 else -1

    def peer(stage, offset):
        mine_at, peer_at, target = [], [], {}
        for axis in (0, 1):
            stride, size = stage[axis]
            digit = lax.rem(place[axis] // stride, size)
            other = lax.rem(digit + offset[axis], size)
            mine_at.append(digit)
            peer_at.append(other)
            target[names[axis]] = place[axis] + (other - digit) * stride
        flat = stage[1][1]
        return mine_at[0] * flat + mine_at[1], peer_at[0] * flat + peer_at[1], target

    levels = levels_of(extent)

    def around(reach, unit, act):
        for dz in range(-reach[0], reach[0] + 1):
            for dx in range(-reach[1], reach[1] + 1):
                far = (unit[0] * dz, unit[1] * dx)
                if far != (0, 0):
                    a, b = place[0] + far[0], place[1] + far[1]

                    @pl.when((a >= 0) & (a < extent[0]) & (b >= 0) & (b < extent[1]))
                    def _():
                        act(at_peer(*far))

    def signal(sem):
        return lambda where: pl.semaphore_signal(
            sem, inc=1, device_id=where, device_id_type=MESH
        )

    def wait_around(sem, reach, unit):
        total = 1
        for axis in (0, 1):
            seen = 1
            for d in range(1, reach[axis] + 1):
                far = d * unit[axis]
                seen = seen + jnp.where(place[axis] >= far, 1, 0)
                seen = seen + jnp.where(place[axis] + far < extent[axis], 1, 0)
            total = total * seen
        pl.semaphore_wait(sem, total - 1)

    def greet(level):
        if 0 < level <= levels:
            unit = tuple(x << (level - 1) for x in REACH)
            wait_around(ready.at[level - 1], (1, 1), unit)
        if level < levels:
            unit = tuple(x << level for x in REACH)
            around((1, 1), unit, signal(ready.at[level]))

    barrier = pltpu.get_barrier_semaphore()
    around(REACH, (1, 1), signal(barrier))

    for kind in (0, 1):
        for side in (0, 1):
            @pl.when(jnp.logical_not(there(kind, side, False)))
            def _():
                halo, coupling = (halo_z, gz_in) if kind == 0 else (halo_x, gx_in)
                for r in range(len(rounds)):
                    for what in (0, 1):
                        halo[r, what, side] = jnp.zeros_like(halo[r, what, side])
                coupling[side] = jnp.zeros_like(coupling[side])
    for sz in (0, 1):
        for sx in (0, 1):
            @pl.when(jnp.logical_not(there(0, sz, False) & there(1, sx, False)))
            def _():
                for r in range(len(rounds)):
                    halo_c[r, sz, sx] = jnp.zeros_like(halo_c[r, sz, sx])

    edge_ref[...] = jnp.zeros_like(edge_ref)
    flat_ref[...] = jnp.zeros_like(flat_ref)
    gz[...] = jnp.zeros_like(gz)
    edge_coef[...] = jnp.zeros_like(edge_coef)
    ee[...] = jnp.zeros_like(ee)
    ee_cross[...] = jnp.zeros_like(ee_cross)
    sums_ref[...] = jnp.zeros_like(sums_ref)
    late_ref[...] = jnp.zeros_like(late_ref)

    def face_copy(r, step, what, kind, side):
        if kind == 0:
            src, dst = send_z.at[r, what, side], halo_z.at[r, what, side]
        else:
            x = width - 1 if side == 0 else 0
            src = allv.at[earlier + step, :, x] if what == 0 else part.at[r, :, x]
            dst = halo_x.at[r, what, side]
        dz, dx = (toward(side), 0) if kind == 0 else (0, toward(side))
        return pltpu.make_async_remote_copy(
            src_ref=src, dst_ref=dst,
            send_sem=face_send.at[what, kind], recv_sem=face_recv.at[r % 2, what, kind],
            device_id=at_peer(dz, dx), device_id_type=MESH,
        )

    def corner_copy(r, sz, sx):
        return pltpu.make_async_remote_copy(
            src_ref=send_c.at[r, sz, sx], dst_ref=halo_c.at[r, sz, sx],
            send_sem=corner_send.at[0], recv_sem=corner_recv.at[r % 2],
            device_id=at_peer(toward(sz), toward(sx)), device_id_type=MESH,
        )

    def g_copy(kind, side):
        if kind == 0:
            src, dst = gz_send.at[side], gz_in.at[side]
        else:
            src = coef_in.at[4, :, :, width - 1] if side == 0 else coef_in.at[3, :, :, 0]
            dst = gx_in.at[side]
        dz, dx = (toward(side), 0) if kind == 0 else (0, toward(side))
        return pltpu.make_async_remote_copy(
            src_ref=src, dst_ref=dst, send_sem=face_send.at[1, kind],
            recv_sem=g_recv.at[kind], device_id=at_peer(dz, dx), device_id_type=MESH,
        )

    def each_face(sending, kinds, act):
        for kind in kinds:
            for side in (0, 1):
                @pl.when(there(kind, side, sending))
                def _():
                    act(kind, side)

    def each_corner(sending, act):
        for sz in (0, 1):
            for sx in (0, 1):
                @pl.when(there(0, sz, sending) & there(1, sx, sending))
                def _():
                    act(sz, sx)

    def amount(ref, send_sem, recv_sem, sending):
        copy = pltpu.make_async_remote_copy(
            src_ref=ref, dst_ref=ref, send_sem=send_sem, recv_sem=recv_sem,
            device_id=at_peer(0, 0), device_id_type=MESH,
        )
        return copy.wait_send if sending else copy.wait_recv

    def both(kind, sending):
        return there(kind, 0, sending) & there(kind, 1, sending)

    def single_side(kind, sending):
        return there(kind, 0, sending) ^ there(kind, 1, sending)

    def wait_faces(r, what, kinds, sending):
        for kind in kinds:
            halo = (halo_z, halo_x)[kind]
            sems = (face_send.at[what, kind], face_recv.at[r % 2, what, kind], sending)
            pl.when(both(kind, sending))(lambda: amount(halo.at[r, what], *sems)())
            pl.when(single_side(kind, sending))(lambda: amount(halo.at[r, what, 0], *sems)())

    def wait_corners(r, sending):
        sems = (corner_send.at[0], corner_recv.at[r % 2], sending)
        two = [both(kind, sending) for kind in (0, 1)]
        one = [single_side(kind, sending) for kind in (0, 1)]
        pl.when(two[0] & two[1])(lambda: amount(halo_c.at[r], *sems)())
        pl.when((two[0] & one[1]) | (one[0] & two[1]))(lambda: amount(halo_c.at[r, 0], *sems)())
        pl.when(one[0] & one[1])(lambda: amount(halo_c.at[r, 0, 0], *sems)())

    def wait_couplings(sending):
        for kind in (0, 1):
            held = (gz_in, gx_in)[kind]
            sems = (face_send.at[1, kind], g_recv.at[kind], sending)
            pl.when(both(kind, sending))(lambda: amount(held, *sems)())
            pl.when(single_side(kind, sending))(lambda: amount(held.at[0], *sems)())

    def pack(r, what, source):
        for e in range(comp):
            for x in range(width):
                row = width * e + x
                tile = source(e, x)
                send_z[r, what, 0, row:row + 1, :] = tile[ROWS - 1:ROWS, :]
                send_z[r, what, 1, row:row + 1, :] = tile[0:1, :]

    def send_faces(r, step):
        pack(r, 0, lambda e, x: allv.at[earlier + step, e, x])
        each_face(True, (0, 1), lambda kind, side: face_copy(r, step, 0, kind, side).start())

    row2 = iota((ROWS, LANES), 0)
    row3 = iota((width, ROWS, LANES), 1)
    lane3 = iota((width, ROWS, LANES), 2)
    zero_tile = jnp.zeros((1, ROWS, LANES), jnp.float32)

    def spread_edges(below, above):
        for e in range(comp):
            for x in range(width):
                at = width * e + x
                edge_ref[e, x:x + 1, :] = below[at:at + 1, :]
                edge_ref[e, 4 + x:5 + x, :] = above[at:at + 1, :]

    def apply_local(step):
        acc = 0.0
        for e in range(comp):
            v = allv[earlier + step, e]
            near = [
                v,
                jnp.where(row3 > 0, pltpu.roll(v, 1, 1), 0.0),
                jnp.where(row3 < ROWS - 1, pltpu.roll(v, ROWS - 1, 1), 0.0),
                jnp.concatenate([zero_tile, v[:-1]], axis=0),
                jnp.concatenate([v[1:], zero_tile], axis=0),
                jnp.where(lane3 > 0, pltpu.roll(v, 1, 2), 0.0),
                jnp.where(lane3 < LANES - 1, pltpu.roll(v, LANES - 1, 2), 0.0),
            ]
            for d in range(len(near)):
                acc = acc + coef[d, :, e] * near[d][None]
        return acc

    def add_x(source, x_of):
        found = []
        for side, d, x in ((0, 3, 0), (1, 4, width - 1)):
            value = source(x)
            for e in range(comp):
                value = value + coef[d, :, e, x] * x_of(side, e)[None]
            found.append(value)
        return found

    def add_z(z_of):
        edge = jnp.zeros((comp, ROWS, LANES), jnp.float32)
        for e in range(comp):
            edge = edge + edge_coef[:, e] * z_of(e)[None]
        return edge

    def store_step(step, source, sides, edge):
        for c in range(comp):
            for x in range(width):
                value = sides[0][c] if x == 0 else sides[1][c] if x == width - 1 else source(x)[c]
                value = value + jnp.where(
                    row2 == 0, edge[c, x:x + 1, :],
                    jnp.where(row2 == ROWS - 1, edge[c, 4 + x:5 + x, :], 0.0),
                )
                allv[earlier + step, c, x] = value

    def take_faces(r, step, source):
        wait_faces(r, 0, (1,), False)
        sides = add_x(source, lambda side, e: halo_x[r, 0, side, e])
        wait_faces(r, 0, (0,), False)
        spread_edges(halo_z.at[r, 0, 0], halo_z.at[r, 0, 1])
        edge = add_z(lambda e: edge_ref[e])
        store_step(step + 1, source, sides, edge)

    def cross_products(k, ref, base):
        total, group = earlier + k + 1, 6
        w = allv[earlier + k]
        for low in range(0, total, group):
            high = min(low + group, total)
            sums = jnp.sum(w[None] * allv[low:high], axis=(1, 2))
            ref[base + low:base + high, :] = jnp.sum(sums, axis=1)

    def as_line(value):
        return jnp.sum(value.T, axis=0, keepdims=True)

    def times(a, b):
        return lax.dot_general(
            a, b, (((1,), (1,)), ((), ())), preferred_element_type=jnp.float32
        )

    def self_products(c):
        parts = split(side_by_side(allv[pl.ds(0, earlier), c]))
        for at, piece in enumerate(parts):
            pieces[at, c] = piece
        one = times(parts[0], parts[0])
        two = times(jnp.concatenate(parts[:2], axis=0), parts[1])
        three = times(parts[0], parts[2])
        span = earlier * ROWS
        ee[...] += one + two[span:]
        ee_cross[...] += two[:span] + three

    def gather_self(value):
        span = earlier * ROWS
        rows = jnp.sum(diagonal(value).reshape(earlier, ROWS, span), axis=1)
        own = onehot((span, LANES), lambda r, q: (r >> 3) == q).astype(jnp.bfloat16)
        found = None
        for piece in split(rows)[::-1]:
            some = lax.dot_general(
                piece, own, (((1,), (0,)), ((), ())), preferred_element_type=jnp.float32
            )
            found = some if found is None else found + some
        return jnp.concatenate(
            [found, jnp.zeros((LANES - earlier, LANES), jnp.float32)], axis=0
        )

    def self_finish():
        cross = gather_self(ee_cross[...])
        whole = gather_self(ee[...])[:32] + (cross + cross.T)[:32]
        packed = whole[:ROWS]
        for g in range(1, 4):
            packed = packed + pltpu.roll(whole[ROWS * g:ROWS * (g + 1)], 32 * g, 1)
        mine_ee[0, :ROWS] = packed
        mine_ee[0, ROWS:] = as_line(sums_ref[0])

    exchanges = {
        "ee": (single, mine_ee, gathered_ee, ee_send, ee_recv),
        "b": (joint, mine_b, gathered_b, b_send, b_recv),
        "f": (joint, mine_f, gathered_f, f_send, f_recv),
    }

    def begin(name, at):
        stages, own, slots, send_sem, recv_sem = exchanges[name]
        for offset in offsets_of(stages[at]):
            here, _, target = peer(stages[at], offset)
            pltpu.make_async_remote_copy(
                src_ref=own.at[at], dst_ref=slots.at[at, here],
                send_sem=send_sem.at[at], recv_sem=recv_sem.at[at],
                device_id=target, device_id_type=MESH,
            ).start()

    def all_of(name, at):
        stages, own, slots, send_sem, recv_sem = exchanges[name]
        others = slots.at[at, pl.ds(0, members(stages[at]) - 1)]
        _, _, target = peer(stages[at], offsets_of(stages[at])[0])
        return pltpu.make_async_remote_copy(
            src_ref=others, dst_ref=others, send_sem=send_sem.at[at], recv_sem=recv_sem.at[at],
            device_id=target, device_id_type=MESH,
        )

    def finish(name, at):
        stages, own, slots, _, _ = exchanges[name]
        here, _, _ = peer(stages[at], (0, 0))
        slots[at, here] = own[at]
        all_of(name, at).wait_recv()
        whole = slots[at, 0]
        for other in range(1, members(stages[at])):
            whole = whole + slots[at, other]
        own[at + 1] = whole

    def drain(name):
        for at in range(len(exchanges[name][0])):
            all_of(name, at).wait_send()

    def whole_exchange(name, first):
        stages = exchanges[name][0]
        for at in range(len(stages)):
            if at or not first:
                begin(name, at)
            finish(name, at)
        return exchanges[name][1][len(stages)] * (1.0 / count)

    def load_height():
        @pl.loop(0, comp)
        def _(c):
            for d in (1, 2):
                coef[d, c] = coef_in[d, c].astype(jnp.float32)
            for e in range(comp):
                for x in range(width):
                    edge_coef[c, e, x:x + 1, :] = coef[1, c, e, x, 0:1, :]
                    edge_coef[c, e, 4 + x:5 + x, :] = coef[2, c, e, x, ROWS - 1:ROWS, :]

        for at in range(comp * comp * width):
            c, e, x = at // (comp * width), at // width % comp, at % width
            flat_ref[0, at:at + 1, :] = edge_coef[c, e, 4 + x:5 + x, :]
            flat_ref[1, at:at + 1, :] = edge_coef[c, e, x:x + 1, :]
        gz_send[...] = flat_ref[...].astype(jnp.bfloat16)

    def load_rest():
        @pl.loop(0, comp)
        def _(c):
            for d in (0, *range(3, coef.shape[0])):
                coef[d, c] = coef_in[d, c].astype(jnp.float32)

    def take_couplings():
        wait_couplings(False)
        flat_ref[...] = gz_in[...].astype(jnp.float32)
        for at in range(comp * comp * width):
            c, e, x = at // (comp * width), at // width % comp, at % width
            gz[c, e, x:x + 1, :] = flat_ref[0, at:at + 1, :]
            gz[c, e, 4 + x:5 + x, :] = flat_ref[1, at:at + 1, :]

    def complete_neighbours(r, step):
        for side, x in ((0, 0), (1, width - 1)):
            for c in range(comp):
                value = jnp.zeros((ROWS, LANES), jnp.float32)
                for e in range(comp):
                    value = value + gx_in[side, c, e].astype(jnp.float32) * allv[earlier + step, e, x]
                pre_x[side, c] = value
        total = jnp.zeros((comp, ROWS, LANES), jnp.float32)
        spread_edges(send_z.at[r, 0, 1], send_z.at[r, 0, 0])
        for e in range(comp):
            total = total + gz[:, e] * edge_ref[e][None]
        pre_z[...] = total
        for sz in (0, 1):
            for sx in (0, 1):
                z = ROWS - 1 if sz == 0 else 0
                x = (4 if sz == 0 else 0) + (width - 1 if sx == 0 else 0)
                for c in range(comp):
                    send_c[r, sz, sx, c:c + 1, :] = pre_x[1 - sx, c, z:z + 1, :]
                    send_c[r, sz, sx, comp + c:comp + c + 1, :] = pre_z[c, x:x + 1, :]
        each_corner(True, lambda sz, sx: corner_copy(r, sz, sx).start())

    def take_ghosts(r, step):
        wait_faces(r, 1, (1, 0), False)
        wait_corners(r, False)
        spread_edges(halo_z.at[r, 1, 0], halo_z.at[r, 1, 1])
        for c in range(comp):
            value = edge_ref[c] + pre_z[c]
            for sz in (0, 1):
                for sx in (0, 1):
                    row = (0 if sz == 0 else 4) + (0 if sx == 0 else width - 1)
                    value = value + jnp.where(row2 == row, halo_c[r, sz, sx, c:c + 1, :], 0.0)
            ghost_z[c] = value
            for side in (0, 1):
                value = halo_x[r, 1, side, c] + pre_x[side, c]
                for sz in (0, 1):
                    row = 0 if sz == 0 else ROWS - 1
                    value = value + jnp.where(
                        row2 == row, halo_c[r, sz, side, comp + c:comp + c + 1, :], 0.0
                    )
                ghost_x[side, c] = value

    with jax.named_scope("start"):
        copy_start.wait()
        copy_early.start()
        wait_around(barrier, REACH, (1, 1))
        greet(0)

    step = 0
    comps = list(range(comp))
    before = max(1, len(rounds) - 1)
    share = [2 * comp // (before + 1)] + [comp // (before + 1)] * (before - 1)
    share[-1] += comp - sum(share)
    share += [0] * (len(rounds) - len(share))
    greeted, ee_at, self_at, done = 1, None, 0, 0

    def self_some(low, high):
        @pl.loop(low, high)
        def _(c):
            self_products(c)

    for r, size in enumerate(rounds):
        with jax.named_scope(f"send{r}"):
            if r:
                wait_faces(r - 1, 0, (0, 1), True)
            send_faces(r, step)
        if r == 0:
            with jax.named_scope("load"):
                copy_height.wait()
                load_height()
                each_face(True, (0,) if paired else (), lambda kind, side: g_copy(kind, side).start())
                for copy in copy_rest:
                    copy.wait()
                each_face(True, (1,) if paired else (), lambda kind, side: g_copy(kind, side).start())
                load_rest()
        with jax.named_scope(f"local{r}"):
            part[r] = apply_local(step)
        with jax.named_scope(f"part{r}"):
            if size == 2:
                pack(r, 1, lambda e, x: part.at[r, e, x])
                if r > paired[0]:
                    wait_faces(r - 1, 1, (0, 1), True)
                else:
                    wait_couplings(True)
                each_face(True, (0, 1), lambda kind, side: face_copy(r, step, 1, kind, side).start())
        with jax.named_scope(f"neigh{r}"):
            if size == 2 and r == paired[0]:
                take_couplings()
            if size == 2:
                if r > paired[0]:
                    wait_corners(r - 1, True)
                complete_neighbours(r, step)
        with jax.named_scope(f"cross{r}"):
            if len(rounds) == 1:
                copy_early.wait()
            if r or len(rounds) == 1:
                for k in range(done, min(step + 1, late)):
                    cross_products(k, sums_ref.at[k // 2], (k % 2) * half)
                    done = k + 1
        with jax.named_scope(f"self{r}"):
            if share[r]:
                middle = self_at + share[r] // 2
                if r == 0:
                    if len(rounds) > 1:
                        copy_early.wait()
                    self_some(self_at, middle)
                    greet(greeted)
                    greeted += 1
                    self_some(middle, self_at + share[r])
                else:
                    if greeted <= levels:
                        greet(greeted)
                        greeted += 1
                    self_some(self_at, self_at + share[r])
                self_at += share[r]
        with jax.named_scope(f"ee{r}"):
            if done == late and r == len(rounds) - 1:
                for q in range(1, lines):
                    mine_b[0, q - 1] = as_line(sums_ref[q])
                begin("b", 0)
            if share[r] and self_at == comp:
                self_finish()
                while greeted <= levels:
                    greet(greeted)
                    greeted += 1
                begin("ee", 0)
                ee_at = 0
            elif ee_at == 0 and len(single) > 1:
                finish("ee", 0)
                begin("ee", 1)
                ee_at = 1
        with jax.named_scope(f"faces{r}"):
            take_faces(r, step, lambda x, r=r: part[r, :, x])
        if size == 2:
            with jax.named_scope(f"late{r}"):
                if r == len(rounds) - 1:
                    cross_products(step + 1, late_ref, 0)
            with jax.named_scope(f"second{r}"):
                acc_ref[...] = apply_local(step + 1)
            with jax.named_scope(f"ghost{r}"):
                take_ghosts(r, step)
            with jax.named_scope(f"store{r}"):
                sides = add_x(lambda x: acc_ref[:, x], lambda side, e: ghost_x[side, e])
                edge = add_z(lambda e: ghost_z[e])
                store_step(step + 2, lambda x: acc_ref[:, x], sides, edge)
        step += size

    with jax.named_scope("last"):
        cross_products(depth, late_ref, half)
        mine_f[0] = as_line(late_ref[...])
        begin("f", 0)

    with jax.named_scope("eewait"):
        for at in range(ee_at, len(single)):
            if at > ee_at:
                begin("ee", at)
            finish("ee", at)
        packed = mine_ee[len(single), :ROWS] * (1.0 / count)
        ahead = mine_ee[len(single), ROWS:] * (1.0 / count)
    row, lane = iota((ROWS, LANES), 0), iota((ROWS, LANES), 1)
    with jax.named_scope("change"):
        copy_shifts.wait()
        unit, nothing = jnp.ones((ROWS, LANES), jnp.float32), jnp.zeros((ROWS, LANES), jnp.float32)
        change = [[unit]]
        for k in range(depth):
            last, scale = change[-1], 1.0 - shifts_ref[k]
            change.append(
                [
                    (last[m - 1] if m else nothing) + (scale * last[m] if m <= k else nothing)
                    for m in range(k + 2)
                ]
            )
        for m in range(block):
            down, along = nothing, nothing
            for k in range(m, block):
                down = jnp.where(row == k, change[k][m], down)
                along = jnp.where(lane == k, change[k][m], along)
            change_ref[0, m] = down
            change_ref[1, m] = along
    with jax.named_scope("bwait"):
        early = whole_exchange("b", True)

    with jax.named_scope("algebra"):
        found = jnp.concatenate(
            [
                pltpu.roll(ahead if k < 2 else early[k // 2 - 1], (k % 2) * half, 1)
                for k in range(late)
            ] + [jnp.zeros((ROWS - late, LANES), jnp.float32)], axis=0
        )
        proj_t = jnp.where(lane < earlier, found, 0.0)
        known = jnp.where(lane < earlier + row, found, 0.0)
        pick = onehot((ROWS, LANES), lambda r, q: q == r + earlier)
        gram = jnp.where(lane <= earlier + row, found, 0.0)
        gram = pltpu.roll(gram, LANES - earlier, 1)[:, :ROWS]
        square = jnp.concatenate(
            [packed] + [pltpu.roll(packed, LANES - 32 * g, 1) for g in range(1, 4)], axis=0
        )
        sr, sl = iota(square.shape, 0), iota(square.shape, 1)
        inside = (sl < earlier) & (sr < earlier)
        square = jnp.where(inside, square - jnp.where(sr == sl, 2.0, 0.0), 0.0)
        moved = dot(proj_t[:, :32], square) + pick
        gram = gram + dot(moved, known, nt=True)

        upper = gram
        inverse = onehot((ROWS, ROWS), lambda r, q: (r == q) & (r < late))
        r8 = iota((ROWS, ROWS), 0)
        q8 = iota((ROWS, ROWS), 1)
        for p in range(late):
            pivot = upper[p:p + 1, p:p + 1]
            scale = inverse_root(pivot)
            column = upper[:, p:p + 1] * scale
            row_u, row_i = upper[p:p + 1, :] * scale, inverse[p:p + 1, :] * scale
            upper = jnp.where(r8 == p, row_u, jnp.where(r8 > p, upper - column * row_u, upper))
            inverse = jnp.where(r8 == p, row_i, jnp.where(r8 > p, inverse - column * row_i, inverse))
        onto = dot(inverse, moved)

        mix = dot(inverse, pick - proj_t)
        tall = jnp.concatenate(
            [jnp.broadcast_to(mix[k:k + 1], (ROWS, LANES)) for k in range(late)], axis=0
        )
        span = earlier * ROWS
        grow = onehot((LANES, span), lambda r, q: (q >> 3) == r).astype(jnp.bfloat16)
        mix = [
            diagonal(
                lax.dot_general(
                    piece, grow, (((1,), (0,)), ((), ())), preferred_element_type=jnp.float32
                )
            ).astype(jnp.bfloat16)
            for piece in split(tall)
        ]
        weights = [
            [
                jnp.broadcast_to(
                    tall[k * ROWS:(k + 1) * ROWS, earlier + i:earlier + i + 1], (ROWS, LANES)
                )
                for i in range(k + 1)
            ]
            for k in range(late)
        ]
    with jax.named_scope("out"):
        for c in range(comp):
            out = dot_pieces(mix, [pieces[at, c] for at in range(3)])
            for x in range(width):
                for k in range(late):
                    value = out[k * ROWS:(k + 1) * ROWS, LANES * x:LANES * (x + 1)]
                    for i in range(k + 1):
                        value = value + weights[k][i] * allv[earlier + i, c, x]
                    new_ref[k, c, x] = value
        proj_early, tri_early = 0.0, 0.0
        for m in range(late):
            proj_early = proj_early + change_ref[0, m] * proj_t[m:m + 1]
            column = jnp.where(r8[:, :1] <= m, upper[:, m:m + 1], 0.0)
            tri_early = tri_early + change_ref[1, m] * column
        small_ref[0:ROWS, :] = proj_early
        small_ref[ROWS:2 * ROWS, :] = jnp.where(row < late, tri_early, 0.0)

    with jax.named_scope("sent"):
        wait_faces(len(rounds) - 1, 0, (0, 1), True)
        if paired:
            wait_faces(paired[-1], 1, (0, 1), True)
            wait_corners(paired[-1], True)
        drain("ee")
        drain("b")
    with jax.named_scope("fwait"):
        final = whole_exchange("f", True)
    with jax.named_scope("columns"):
        ys = [final, pltpu.roll(final, half, 1)][2 - (block - late):]
        spread = [jnp.broadcast_to(y, (ROWS, LANES)) for y in ys]
        tiles = -(-(earlier + block) // ROWS)
        columns = []
        for y in spread:
            col = [
                lane_sums(jnp.where(lane == row + ROWS * t, y, 0.0)) for t in range(tiles)
            ]
            img = [
                lane_sums(square[ROWS * t:ROWS * (t + 1)] * y) for t in range(square.shape[0] // ROWS)
            ]
            columns.append((col, img, lane_sums(onto * y)))
        wide = lambda value: jnp.broadcast_to(value, (ROWS, LANES))

        def inner(a, b):
            (col_a, _, r_a), (col_b, img_b, r_b) = columns[a], columns[b]
            total = -(r_a * r_b)
            for t in range(len(img_b)):
                total = total + jnp.where(row[:, :1] + ROWS * t < earlier, col_a[t] * img_b[t], 0.0)
            for t in range(tiles):
                total = total + jnp.where(row[:, :1] + ROWS * t == earlier + late + a, col_b[t], 0.0)
            return sublane_sums(wide(total))

        fresh = block - late
        scales, ratios, lines_out = [], {}, []
        for b in range(fresh):
            value = inner(b, b)
            for a in range(b):
                cross = inner(a, b)
                ratios[a, b] = cross * scales[a]
                value = value - ratios[a, b] * ratios[a, b]
            scales.append(inverse_root(value))
            ratios[b, b] = value * scales[b]
        triangle = small_ref[ROWS:2 * ROWS, :]
        proj_rows = small_ref[0:ROWS, :]
        for b in range(fresh):
            column = wide(columns[b][2])
            for a in range(b + 1):
                column = jnp.where(row == late + a, ratios[a, b], column)
            triangle = triangle + change_ref[1, late + b] * column
            proj_rows = proj_rows + change_ref[0, late + b] * spread[b]
        small_ref[ROWS:2 * ROWS, :] = triangle
        small_ref[0:ROWS, :] = proj_rows
        for b in range(fresh):
            for t in range(tiles):
                late_ref[b * half + ROWS * t:b * half + ROWS * (t + 1), :] = wide(columns[b][0][t])
            late_ref[b * half + ROWS * tiles:b * half + ROWS * (tiles + 1), :] = wide(columns[b][2])

    with jax.named_scope("tail"):
        for c in range(comp):
            totals = [allv[earlier + late + b, c] for b in range(fresh)]
            for j in range(earlier):
                v = allv[j, c]
                for b in range(fresh):
                    at = b * half + j
                    totals[b] = totals[b] - late_ref[at:at + 1, :] * v
            for i in range(late):
                v = new_ref[i, c]
                for b in range(fresh):
                    at = b * half + ROWS * tiles + i
                    totals[b] = totals[b] - late_ref[at:at + 1, :] * v
            outs = []
            for b in range(fresh):
                value = totals[b]
                for a in range(b):
                    value = value - ratios[a, b] * outs[a]
                outs.append(value * scales[b])
                new_ref[late + b, c] = outs[b]

    with jax.named_scope("drain"):
        drain("f")
        proj_ref[...] = small_ref[:block, :earlier]
        tri_ref[...] = small_ref[ROWS:ROWS + block, :block]


def hand_over(new_in, proj_in, tri_in, new_out, proj_out, tri_out, sem):
    pairs = ((new_in, new_out), (proj_in, proj_out), (tri_in, tri_out))
    copies = [pltpu.make_async_copy(*pair, sem.at[at]) for at, pair in enumerate(pairs)]
    for copy in copies:
        copy.start()
    for copy in copies:
        copy.wait()


def body(sizes, coefficients, earlier, start, shifts):
    coefficients = jnp.transpose(coefficients, (0, 1, 2, 4, 3, 5))
    earlier = jnp.transpose(earlier, (0, 1, 3, 2, 4))
    start = jnp.transpose(start, (0, 2, 1, 3))
    depth, count = shifts.shape[0], earlier.shape[0]
    block = depth + 1
    kinds, comp, _, width, rows, lanes = coefficients.shape
    rounds = len(steps_of(depth))
    flat = -(-comp * comp * width // 16) * 16
    late = block - steps_of(depth)[-1]
    lines = late // 2 + late % 2
    single, joint = stages_of(sizes), joint_stages_of(sizes)
    most = max(members(stage) for stage in single)
    joined = max(members(stage) for stage in joint)
    levels = max(1, levels_of([n for _, n in sizes]))
    f32, b16 = jnp.float32, jnp.bfloat16
    anywhere = pl.BlockSpec(memory_space=pl.ANY)
    vmem = pl.BlockSpec(memory_space=pltpu.VMEM)
    sems = pltpu.SemaphoreType.DMA
    found = pl.pallas_call(
        functools.partial(kernel, sizes),
        out_shape=(
            pltpu.VMEM((block, comp, width, rows, lanes), f32),
            pltpu.VMEM((block, count), f32),
            pltpu.VMEM((block, block), f32),
        ),
        in_specs=[anywhere] * 4,
        out_specs=(vmem, vmem, vmem),
        scratch_shapes=[
            pltpu.VMEM(coefficients.shape, coefficients.dtype),
            pltpu.VMEM(coefficients.shape, f32),
            pltpu.VMEM((comp, comp, rows, lanes), f32),
            pltpu.VMEM((2, comp, comp, rows, lanes), b16),
            pltpu.VMEM((2, flat, lanes), b16),
            pltpu.VMEM((2, flat, lanes), b16),
            pltpu.VMEM((2, flat, lanes), f32),
            pltpu.VMEM((comp, comp, rows, lanes), f32),
            pltpu.VMEM((count + block, comp, width, rows, lanes), f32),
            pltpu.VMEM((3, comp, count * rows, width * lanes), b16),
            pltpu.VMEM((rounds, comp, width, rows, lanes), f32),
            pltpu.VMEM((comp, width, rows, lanes), f32),
            pltpu.VMEM((rounds, 2, 2, comp, rows, lanes), f32),
            pltpu.VMEM((rounds, 2, 2, width * comp, lanes), f32),
            pltpu.VMEM((rounds, 2, 2, width * comp, lanes), f32),
            pltpu.VMEM((rounds, 2, 2, 2 * comp, lanes), f32),
            pltpu.VMEM((rounds, 2, 2, 2 * comp, lanes), f32),
            pltpu.VMEM((2, comp, rows, lanes), f32),
            pltpu.VMEM((comp, rows, lanes), f32),
            pltpu.VMEM((2, comp, rows, lanes), f32),
            pltpu.VMEM((comp, rows, lanes), f32),
            pltpu.VMEM((comp, rows, lanes), f32),
            pltpu.VMEM((count * rows, count * rows), f32),
            pltpu.VMEM((count * rows, count * rows), f32),
            pltpu.VMEM((lines, lanes, lanes), f32),
            pltpu.VMEM((lanes, lanes), f32),
            pltpu.VMEM((2 * rows, lanes), f32),
            pltpu.VMEM((2, block, rows, lanes), f32),
            pltpu.VMEM((len(single) + 1, rows + 1, lanes), f32),
            pltpu.VMEM((len(single), most, rows + 1, lanes), f32),
            pltpu.VMEM((len(joint) + 1, max(1, lines - 1), 1, lanes), f32),
            pltpu.VMEM((len(joint), joined, max(1, lines - 1), 1, lanes), f32),
            pltpu.VMEM((len(joint) + 1, 1, lanes), f32),
            pltpu.VMEM((len(joint), joined, 1, lanes), f32),
            sems((6,)),
            sems((2, 2)),
            sems((2, 2, 2)),
            sems((1,)),
            sems((2,)),
            sems((2,)),
            sems((len(single),)),
            sems((len(single),)),
            sems((len(joint),)),
            sems((len(joint),)),
            sems((len(joint),)),
            sems((len(joint),)),
            pltpu.SemaphoreType.REGULAR((levels,)),
            pltpu.SMEM(shifts.shape, f32),
        ],
        compiler_params=pltpu.CompilerParams(collective_id=0, has_side_effects=True),
        name="powers",
    )(coefficients, earlier, start, shifts)
    found = [pltpu.with_memory_space_constraint(value, pltpu.VMEM) for value in found]
    new, proj, tri = pl.pallas_call(
        hand_over,
        out_shape=[jax.ShapeDtypeStruct(value.shape, f32) for value in found],
        in_specs=[vmem] * 3,
        out_specs=[anywhere] * 3,
        scratch_shapes=[sems((3,))],
        name="hand_over",
    )(*found)
    return jnp.transpose(new, (0, 1, 3, 2, 4)), proj.T, tri


def solution(mesh):
    sizes = (("slab", mesh.shape["slab"]), ("sub", mesh.shape["sub"]))
    placed = (
        P(None, None, None, "slab", "sub", None),
        P(None, None, "slab", "sub", None),
        P(None, "slab", "sub", None),
        P(),
    )
    return jax.shard_map(
        functools.partial(body, sizes),
        mesh=mesh,
        in_specs=placed,
        out_specs=(P(None, None, "slab", "sub", None), P(), P()),
        check_vma=False,
    )
```
